32 devices in a mesh: row: 8 (over z, core), col: 4 (over y, x).
Axes of the slice: x: 2, y: 2, z: 4, core: 2. Of those that a mesh axis runs over, the one named last changes fastest.
Arguments:
- x_fwd: bfloat16 [512, 6144], P('row', 'col'), may hold values from -6 to 6
- x_bwd: bfloat16 [512, 6144], P('row', 'col'), may hold values from -6 to 6
- grad_out: bfloat16 [512, 6144], P('row', 'col'), may hold values from -1.5 to 1.5
- gain: float32 [6144], P('col'), may hold values from 0.1 to 1.9
- w_up: bfloat16 [6144, 12288], P('col', 'row'), may hold values from -0.078125 to 0.078125
- w_down: bfloat16 [12288, 6144], P('row', 'col'), may hold values from -0.0546875 to 0.0546875
Outputs:
- y_fwd: bfloat16 [512, 6144], P('row', 'col')
- dx_bwd: bfloat16 [512, 6144], P('row', 'col')
- step_up: float32 [6144, 12288], P('col', 'row')
- step_down: float32 [12288, 6144], P('row', 'col')
- step_gain: float32 [6144], P('col')
- grad_rms: float32 [], replicated
The draws below stay inside these ranges and needn't reach their ends.
All inputs are finite; a program needn't handle non-finite values.
Results may differ from the reference program's by a relative error of at most 0.0017.
The reference program's roundings to bfloat16 on the way count: a program that leaves them out, or rounds other values in their place, can miss the bound.
Values may be sent and summed in bfloat16 or wider, within the bound.
A program may use at most 128 MiB of HBM per device.

```python
import math
import jax
import jax.numpy as jnp
from jax import lax

D = 6144
FF = 12288
TOKENS = 512
PARAMS = 151001088


def steps_of(key, dims, pieces, smallest, high):
    level, own = 1.0, jax.random.fold_in(key, 6)
    for dim, shards_of in pieces:
        draws = jnp.exp(jax.random.uniform(jax.random.fold_in(own, dim), (shards_of,), jnp.float32, smallest / len(pieces), high / len(pieces)))
        level = level * jnp.repeat(draws, dims[dim] // shards_of).reshape([-1 if axis == dim else 1 for axis in range(len(dims))])
    return level


def bell_draw(rng, dims, scale, reach, split=(), held_as=jnp.bfloat16):
    drawn = jax.random.normal(rng, dims, jnp.float32) * scale
    if len(split) > 0:
        drawn = steps_of(rng, dims, split, -0.22, 0.18) * drawn
    return jnp.clip(drawn, min=-reach, max=reach).astype(held_as)


def setup_inputs(seed: int = 0) -> dict:
    arg_keys = jax.random.split(jax.random.key(seed), 7)
    return {
        "x_fwd": bell_draw(arg_keys[0], (TOKENS, D), 1.0, 6.0, ((0, 8), (1, 4))),
        "x_bwd": bell_draw(arg_keys[1], (TOKENS, D), 1.0, 6.0, ((0, 8), (1, 4))),
        "grad_out": bell_draw(arg_keys[2], (TOKENS, D), 0.25, 1.5, ((0, 8), (1, 4))),
        "gain": jnp.clip(1.0 + 0.18 * jax.random.normal(arg_keys[3], (D,), jnp.float32), 0.1, 1.9),
        "w_up": bell_draw(arg_keys[4], (D, FF), D ** -0.5, 0.078125, ((0, 4), (1, 8))),
        "w_down": bell_draw(arg_keys[5], (FF, D), FF ** -0.5, 0.0546875, ((0, 8), (1, 4))),
    }


eps = 1e-06
clip_share = 0.25

def erf_gelu(value):
    return 0.5 * value * (1.0 + lax.erf(value * 0.7071067811865476))

def gelu_slope(value):
    return 0.5 * (1.0 + lax.erf(value * 0.7071067811865476)) + value * jnp.exp(-0.5 * value * value) * 0.3989422804014327

def normalize(tokens):
    values = tokens.astype(jnp.float32)
    width = values.shape[-1]
    centre = lax.optimization_barrier(jnp.sum(values, -1, keepdims=True)) / width
    spread = lax.optimization_barrier(jnp.sum(values * values, -1, keepdims=True)) / width - centre * centre
    inv_scale = lax.rsqrt(spread + eps)
    return ((values - centre) * inv_scale, inv_scale)

def reference(x_fwd, x_bwd, grad_out, gain, w_up, w_down):
    centred_a, _ = normalize(x_fwd)
    normed_a = (centred_a * gain).astype(jnp.bfloat16)
    pre_a = jnp.dot(normed_a, w_up, preferred_element_type=jnp.float32)
    hidden_a = erf_gelu(pre_a).astype(jnp.bfloat16)
    y_fwd = (x_fwd.astype(jnp.float32) + jnp.dot(hidden_a, w_down, preferred_element_type=jnp.float32)).astype(jnp.bfloat16)
    centred_b, inv_scale = normalize(x_bwd)
    normed_b = (centred_b * gain).astype(jnp.bfloat16)
    pre_b = jnp.dot(normed_b, w_up, preferred_element_type=jnp.float32)
    hidden_b = erf_gelu(pre_b).astype(jnp.bfloat16)
    grad_hidden = jnp.dot(grad_out, w_down.T, preferred_element_type=jnp.float32)
    grad_pre = (grad_hidden * gelu_slope(pre_b)).astype(jnp.bfloat16)
    g_down = jnp.dot(hidden_b.T, grad_out, preferred_element_type=jnp.float32)
    g_up = jnp.dot(normed_b.T, grad_pre, preferred_element_type=jnp.float32)
    grad_normed = jnp.dot(grad_pre, w_up.T, preferred_element_type=jnp.float32)
    g_gain = lax.optimization_barrier(jnp.sum(grad_normed * centred_b, 0))
    scaled = grad_normed * gain
    width = scaled.shape[-1]
    first = lax.optimization_barrier(jnp.sum(scaled, -1, keepdims=True)) / width
    second = lax.optimization_barrier(jnp.sum(scaled * centred_b, -1, keepdims=True)) / width
    dx_bwd = (grad_out.astype(jnp.float32) + inv_scale * (scaled - first - centred_b * second)).astype(jnp.bfloat16)
    total = jnp.sum(g_up * g_up) + jnp.sum(g_down * g_down) + jnp.sum(g_gain * g_gain)
    norm_value = jnp.sqrt(total)
    grad_rms = norm_value / math.sqrt(PARAMS)
    factor = jnp.minimum(1.0, clip_share * math.sqrt(PARAMS) / norm_value)
    return (y_fwd, dx_bwd, g_up * factor, g_down * factor, g_gain * factor, grad_rms)
```

```python
import functools
import math

import jax
import jax.numpy as jnp
from jax import lax
from jax.experimental import pallas as pl
from jax.experimental.pallas import tpu as pltpu
from jax.sharding import PartitionSpec as P

D = 6144
FF = 12288


eps = 1e-06
clip_share = 0.25


def erf_gelu(value):
    return 0.5 * value * (1.0 + lax.erf(value * 0.7071067811865476))


def gelu_slope(value):
    return (
        0.5 * (1.0 + lax.erf(value * 0.7071067811865476))
        + value * jnp.exp(-0.5 * value * value) * 0.3989422804014327
    )


def contract(left, right, left_dim, right_dim):
    return lax.dot_general(
        left, right, (((left_dim,), (right_dim,)), ((), ())), preferred_element_type=jnp.float32
    )


def row_sums(tokens):
    values = tokens.astype(jnp.float32)
    return (jnp.sum(values, -1), jnp.sum(values * values, -1))


def normalize(tokens, first, second):
    values = tokens.astype(jnp.float32)
    centre = first / D
    spread = second / D - centre * centre
    inv_scale = lax.rsqrt(spread + eps)
    return ((values - centre[:, None]) * inv_scale[:, None], inv_scale)


def up_both(normed_a, normed_b, w_up):
    full_a, full_b = (
        lax.all_gather(normed_a, "row", axis=0, tiled=True),
        lax.all_gather(normed_b, "row", axis=0, tiled=True),
    )
    width = w_up.shape[1]
    summed = lax.psum_scatter(
        jnp.concatenate(
            [
                jnp.dot(full_a, w_up, preferred_element_type=jnp.float32),
                jnp.dot(full_b, w_up, preferred_element_type=jnp.float32),
            ],
            1,
        ),
        "col",
        scatter_dimension=0,
        tiled=True,
    )
    return (summed[:, :width], summed[:, width:], full_b)


def on_device(x_fwd, x_bwd, grad_out, gain, w_up, w_down):
    first_a, second_a = row_sums(x_fwd)
    first_b, second_b = row_sums(x_bwd)
    first_a, second_a, first_b, second_b = lax.psum((first_a, second_a, first_b, second_b), "col")
    centred_a, _ = normalize(x_fwd, first_a, second_a)
    centred_b, inv_scale = normalize(x_bwd, first_b, second_b)
    normed_a = (centred_a * gain).astype(jnp.bfloat16)
    normed_b = (centred_b * gain).astype(jnp.bfloat16)
    pre_a, pre_b, normed_full = up_both(normed_a, normed_b, w_up)
    hidden_a = erf_gelu(pre_a).astype(jnp.bfloat16)
    output_part = jnp.dot(
        lax.all_gather(hidden_a, "col", axis=0, tiled=True),
        w_down,
        preferred_element_type=jnp.float32,
    )
    output_sum = lax.psum_scatter(output_part, "row", scatter_dimension=0, tiled=True)
    y_fwd = (x_fwd.astype(jnp.float32) + output_sum).astype(jnp.bfloat16)
    hidden_b = erf_gelu(pre_b).astype(jnp.bfloat16)
    grad_full = lax.all_gather(grad_out, "row", axis=0, tiled=True)
    grad_hidden = lax.psum_scatter(
        contract(grad_full, w_down, 1, 1), "col", scatter_dimension=0, tiled=True
    )
    grad_pre = (grad_hidden * gelu_slope(pre_b)).astype(jnp.bfloat16)
    hidden_piece = lax.all_gather(hidden_b, "col", axis=0, tiled=True)
    pre_piece = lax.all_gather(grad_pre, "col", axis=0, tiled=True)
    down_total = contract(hidden_piece, grad_full, 0, 0)
    up_total = contract(normed_full, pre_piece, 0, 0)
    input_total = contract(pre_piece, w_up, 1, 1)
    grad_normed = lax.psum_scatter(input_total, "row", scatter_dimension=0, tiled=True)
    scaled = grad_normed * gain
    first_back = jnp.sum(scaled, -1)
    second_back = jnp.sum(scaled * centred_b, -1)
    first_back, second_back = lax.psum((first_back, second_back), "col")
    dx_bwd = (
        grad_out.astype(jnp.float32)
        + inv_scale[:, None]
        * (scaled - first_back[:, None] / D - centred_b * (second_back[:, None] / D))
    ).astype(jnp.bfloat16)
    gain_part = jnp.sum(grad_normed * centred_b, 0)
    weight_squares = jnp.sum(up_total * up_total) + jnp.sum(down_total * down_total)
    g_gain = lax.psum(gain_part, "row")
    first_row = (lax.axis_index("row") == 0).astype(jnp.float32)
    total = lax.psum(weight_squares + first_row * jnp.sum(g_gain * g_gain), ("row", "col"))
    param_count = 2 * D * FF + D
    norm_value = jnp.sqrt(total)
    grad_rms = norm_value / math.sqrt(param_count)
    factor = jnp.minimum(1.0, clip_share * math.sqrt(param_count) / norm_value)
    return (y_fwd, dx_bwd, up_total * factor, down_total * factor, g_gain * factor, grad_rms)


MESH = pl.DeviceIdType.MESH
VMEM = pl.BlockSpec(memory_space=pltpu.VMEM)
F32 = jnp.float32
BF16 = jnp.bfloat16
DMA = pltpu.SemaphoreType.DMA
GRANT = 60 * 1024 * 1024


def greet(peers):
    barrier = pltpu.get_barrier_semaphore()
    for peer in peers:
        pl.semaphore_signal(barrier, inc=1, device_id=peer, device_id_type=MESH)
    pl.semaphore_wait(barrier, len(peers))


def send(src, dst, send_sem, recv_sem, peer):
    return pltpu.make_async_remote_copy(
        src_ref=src, dst_ref=dst, send_sem=send_sem, recv_sem=recv_sem,
        device_id=peer, device_id_type=MESH,
    )


def arrived(ref, sem, peer):
    pltpu.make_async_remote_copy(
        src_ref=ref, dst_ref=ref, send_sem=sem, recv_sem=sem,
        device_id=peer, device_id_type=MESH,
    ).wait_recv()


SPAN = 252.0


def encode(values):
    size = jnp.abs(values)
    peak = jnp.maximum(jnp.max(size, 0, keepdims=True), 1e-30)
    code = jnp.exp2(size * (SPAN / peak) - 0.5 * SPAN)
    return jnp.where(values < 0.0, -code, code).astype(BF16), peak


def decode(codes, peak):
    code = codes.astype(F32)
    size = jnp.log(jnp.abs(code)) * (peak * (1.4426950408889634 / SPAN)) + 0.5 * peak
    return jnp.where(code < 0.0, -size, size)


def normal_of(values, stats, at, width):
    centre = stats[:, at : at + 1] / width
    spread = stats[:, at + 1 : at + 2] / width - centre * centre
    inv = lax.rsqrt(spread + eps)
    return (values - centre) * inv, inv


def lanes_of(columns):
    rows = columns[0].shape[0]
    lane = lax.broadcasted_iota(jnp.int32, (rows, 128), 1)
    out = jnp.zeros((rows, 128), F32)
    for i, column in enumerate(columns):
        out = jnp.where(lane == i, column, out)
    return out


def layer_kernel(R, C, width, xa, xb, go, gain, w_up_hbm, w_down_hbm, full, stats, acts, sums,
                 w_up, w_down, st_own, st_in, out_send, buf, inb, buf_p, inb_p, hold, own,
                 part, from_sib, zbuf, zin, zbuf_p, zin_p,
                 w_sem, st_send, st_recv, s_right, s_left, s_sib, recv, sem_s, sem_r, pk_s, pk_r,
                 g_s, g_r, sib_s, sib_r, z_s, z_r, zp_s, zp_r):
    row, col = lax.axis_index("row"), lax.axis_index("col")
    chips = R // 2
    chip, core = row // 2, row % 2
    sib = {"row": row + 1 - 2 * core, "col": col}

    def line(step):
        return {"row": row + 2 * step, "col": col}

    cols = [{"row": row, "col": (col + i) % C} for i in range(1, C)]
    flip_x = col + 1 - 2 * (col % 2)
    flip_y = (col + 2) % 4
    diag = 3 - col
    peer_x, peer_y = {"row": row, "col": flip_x}, {"row": row, "col": flip_y}
    share = xa.shape[0]
    tokens, wide = out_send.shape[1], out_send.shape[2]
    half = wide // 2
    tile = half // 2
    load_up = pltpu.make_async_copy(w_up_hbm, w_up, w_sem.at[0])
    load_down = pltpu.make_async_copy(w_down_hbm, w_down, w_sem.at[1])
    load_down.start()
    load_up.start()
    greet(cols + [sib] + [{"row": (row + 2 * i) % R, "col": col} for i in range(1, chips)])

    def block(j, owner):
        return full.at[j, pl.ds(owner * share, share), :]

    def spread(j, owner, slot, src, to_right, to_left):
        dst = block(j, owner)
        out = [(None, send(src, dst, s_sib.at[j, slot], recv.at[j, owner], sib))]
        if to_right:
            out.append((chip < chips - 1,
                        send(src, dst, s_right.at[j, slot], recv.at[j, owner], line(1))))
        if to_left:
            out.append((chip > 0,
                        send(src, dst, s_left.at[j, slot], recv.at[j, owner], line(-1))))
        return out

    def start(copies):
        for cond, copy in copies[::-1]:
            if cond is None:
                copy.start()
            else:
                pl.when(cond)(copy.start)

    def finish(copies):
        for cond, copy in copies:
            if cond is None:
                copy.wait_send()
            else:
                pl.when(cond)(copy.wait_send)

    mine = {2: spread(2, row, 0, go, True, True)}
    start(mine[2])
    a, b = xa[...].astype(F32), xb[...].astype(F32)
    moments = []
    for v in (a, b):
        moments += [jnp.sum(v, 1, keepdims=True), jnp.sum(v * v, 1, keepdims=True)]
    st_own[...] = lanes_of(moments)
    st_copies = [send(st_own, st_in.at[i], st_send.at[i], st_recv.at[i], p)
                 for i, p in enumerate(cols)]
    for copy in st_copies:
        copy.start()
    block(2, row)[...] = go[...]
    for copy in st_copies:
        copy.wait()
    total = st_own[...]
    for i in range(C - 1):
        total = total + st_in[i]
    stats[...] = total
    for j, x, at in ((1, xb, 2), (0, xa, 0)):
        hat, _ = normal_of(x[...].astype(F32), total, at, width)
        block(j, row)[...] = (hat * gain[...]).astype(BF16)
        mine[j] = spread(j, row, 0, block(j, row), True, True)
        start(mine[j])

    def relays(j, visit):
        for step in range(1, chips):
            for sign in (-1, 1):
                ok = chip >= step if sign < 0 else chip + step < chips

                @pl.when(ok)
                def _():
                    owner = row + 2 * sign * step
                    slot = step if sign < 0 else chips - 1 + step
                    visit(owner, sign, spread(j, owner, slot, block(j, owner), sign < 0, sign > 0))

    def gathered(j):
        def visit(owner, sign, copies):
            arrived(block(j, owner), recv.at[j, owner], line(sign))
            start(copies)

        relays(j, visit)
        for chip_of in range(chips):
            owner = 2 * chip_of + 1 - core
            arrived(block(j, owner), recv.at[j, owner], sib)

    def multiply(j, q, h, put):
        @pl.loop(0, half // tile)
        def _(t):
            at = pl.ds(pl.multiple_of(h * half + t * tile, tile), tile)
            left = full[j, pl.ds(q * tokens, tokens), :]
            if j == 2:
                piece = lax.dot_general(left, w_down[at, :], (((1,), (1,)), ((), ())),
                                        preferred_element_type=F32)
            else:
                piece = jnp.dot(left, w_up[:, at], preferred_element_type=F32)
            put(pl.ds(pl.multiple_of(t * tile, tile), tile), piece)

    def into(j, s):
        def put(at, piece):
            buf[j, s, :, at], buf_p[j, s, :, at] = encode(piece)
        return put

    def keep(ref, j, h):
        def put(at, piece):
            ref[j, h, :, at] = piece
        return put

    target = (peer_x, peer_y, peer_x, peer_x, peer_y, peer_y)

    def hop(j, s):
        return (send(buf.at[j, s], inb.at[j, s], sem_s.at[j, s], sem_r.at[j, s], target[s]),
                send(buf_p.at[j, s], inb_p.at[j, s], pk_s.at[j, s], pk_r.at[j, s], target[s]))

    def go_hop(j, s):
        for copy in hop(j, s):
            copy.start()

    def got_hop(j, s):
        for copy in hop(j, s):
            copy.wait_recv()

    def products(j):
        multiply(j, diag, 0, into(j, 0))
        go_hop(j, 0)
        multiply(j, diag, 1, into(j, 1))
        go_hop(j, 1)
        multiply(j, flip_x, 0, into(j, 2))
        go_hop(j, 2)
        multiply(j, flip_y, 1, into(j, 5))
        go_hop(j, 5)
        multiply(j, flip_y, 0, keep(hold, j, 0))
        multiply(j, flip_x, 1, keep(hold, j, 1))
        multiply(j, col, 0, keep(own, j, 0))
        multiply(j, col, 1, keep(own, j, 1))

    def transit(j):
        for s, onward_s in ((0, 4), (1, 3)):
            got_hop(j, s)
            @pl.loop(0, half // tile)
            def _(t):
                at = pl.ds(pl.multiple_of(t * tile, tile), tile)
                merged = hold[j, s, :, at] + decode(inb[j, s, :, at], inb_p[j, s, :, at])
                buf[j, onward_s, :, at], buf_p[j, onward_s, :, at] = encode(merged)
            go_hop(j, onward_s)

    def landed(j):
        for s in range(2, 6):
            got_hop(j, s)

    def summed(j, h, at):
        return (own[j, h, at, :] + decode(inb[j, 2 + h, at, :], inb_p[j, 2 + h])
                + decode(inb[j, 4 + h, at, :], inb_p[j, 4 + h]))

    chunk = 16

    def over(body):
        @pl.loop(0, tokens // chunk)
        def _(i):
            for h in range(2):
                body(h, pl.ds(pl.multiple_of(i * chunk, chunk), chunk))

    def first(k, which):
        peer = (peer_x, peer_y)[which]
        return send(out_send.at[k], acts.at[k, pl.ds(col * tokens, tokens), :], g_s.at[k, which], g_r.at[k, which], peer)

    def relay(k, which):
        owner = (flip_x, flip_y)[which]
        ref = acts.at[k, pl.ds(owner * tokens, tokens), pl.ds(which * half, half)]
        return send(ref, ref, g_s.at[k, 2 + which], g_r.at[k, 2 + which], (peer_y, peer_x)[which])

    def publish(k):
        first(k, 0).start()
        first(k, 1).start()

    def pass_on(k):
        first(k, 0).wait_recv()
        relay(k, 0).start()
        first(k, 1).wait_recv()
        relay(k, 1).start()

    def backward(h, at):
        v = summed(1, h, at)
        phi = 0.5 * (1.0 + lax.erf(v * 0.7071067811865476))
        g = summed(2, h, at)
        slope = phi + v * jnp.exp(-0.5 * v * v) * 0.3989422804014327
        out_send[1, at, h * half : (h + 1) * half] = (v * phi).astype(BF16)
        out_send[2, at, h * half : (h + 1) * half] = (g * slope).astype(BF16)

    def forward(h, at):
        v = summed(0, h, at)
        out_send[0, at, h * half : (h + 1) * half] = (
            0.5 * v * (1.0 + lax.erf(v * 0.7071067811865476))).astype(BF16)

    rows, broad = sums.shape[1], sums.shape[2]
    step_n = broad // 4
    order = []
    low, high = 0, chips - 1
    while low <= high:
        order.append(high)
        if low < high:
            order.append(low)
        low, high = low + 1, high - 1

    def to_sib(j, z):
        return send(part.at[j, z, 1 - core], from_sib.at[j, z], sib_s.at[j, z], sib_r.at[j, z], sib)

    def to_owner(j, z):
        peer = {"row": 2 * z + core, "col": col}
        return (send(zbuf.at[j, z], zin.at[j, chip], z_s.at[j, z], z_r.at[j, chip], peer),
                send(zbuf_p.at[j, z], zin_p.at[j, chip], zp_s.at[j, z], zp_r.at[j, chip], peer))

    def product(j, z):
        @pl.loop(0, broad // step_n)
        def _(t):
            at = pl.ds(pl.multiple_of(t * step_n, step_n), step_n)
            left = acts[2 * j, pl.ds(z * 2 * rows, 2 * rows), :]
            if j == 0:
                piece = jnp.dot(left, w_down[:, at], preferred_element_type=F32)
            else:
                piece = lax.dot_general(left, w_up[at, :], (((1,), (1,)), ((), ())),
                                        preferred_element_type=F32)
            part[j, z, 0, :, at] = piece[:rows]
            part[j, z, 1, :, at] = piece[rows:]
        to_sib(j, z).start()

    def onward(j, z):
        to_sib(j, z).wait_recv()

        @pl.when(z != chip)
        def _():
            @pl.loop(0, broad // step_n)
            def _(t):
                at = pl.ds(pl.multiple_of(t * step_n, step_n), step_n)
                zbuf[j, z, :, at], zbuf_p[j, z, :, at] = encode(
                    part[j, z, core, :, at] + from_sib[j, z, :, at])
            for copy in to_owner(j, z):
                copy.start()

    def complete(k):
        for which in (0, 1):
            ref = acts.at[k, pl.ds(diag * tokens, tokens), pl.ds(which * half, half)]
            arrived(ref, g_r.at[k, 2 + which], (peer_y, peer_x)[which])

    gathered(2)
    load_down.wait()
    products(2)
    gathered(1)
    load_up.wait()
    products(1)
    transit(2)
    gathered(0)
    products(0)
    transit(1)
    landed(2)
    landed(1)
    transit(0)
    over(backward)
    publish(2)
    landed(0)
    over(forward)
    publish(0)
    for k in (2, 0, 1):
        acts[k, pl.ds(col * tokens, tokens), :] = out_send[k]
    pass_on(2)
    publish(1)
    complete(2)
    for z in order:
        product(1, z)
    pass_on(0)
    complete(0)
    for z in order:
        onward(1, z)
        product(0, z)
    pass_on(1)
    for z in order:
        onward(0, z)
    complete(1)
    for j in (2, 1, 0):
        finish(mine[j])
        relays(j, lambda owner, sign, copies: finish(copies))
        for which in (0, 1):
            relay(j, which).wait_send()
            first(j, which).wait_send()
        for s in range(6):
            for copy in hop(j, s):
                copy.wait_send()
    for j in (0, 1):
        sums[j] = part[j, chip, core] + from_sib[j, chip]
        for z in range(chips):
            @pl.when(z != chip)
            def _():
                peer = {"row": 2 * z + core, "col": col}
                arrived(zin.at[j, z], z_r.at[j, z], peer)
                arrived(zin_p.at[j, z], zp_r.at[j, z], peer)
                sums[j] = sums[j] + decode(zin[j, z], zin_p[j, z])

    for j in (0, 1):
        for z in range(chips):
            to_sib(j, z).wait_send()

            @pl.when(z != chip)
            def _():
                for copy in to_owner(j, z):
                    copy.wait_send()


def layer(R, C, width, x_fwd, x_bwd, grad_out, gain, w_up, w_down):
    rows, columns = x_fwd.shape
    wide = w_up.shape[1]
    chips, slots = R // 2, 2 * (R // 2) - 1
    count = rows * R
    tokens, half = count // C, wide // 2
    return pl.pallas_call(
        functools.partial(layer_kernel, R, C, width),
        out_shape=(jax.ShapeDtypeStruct((3, count, columns), BF16),
                   jax.ShapeDtypeStruct((rows, 128), F32),
                   jax.ShapeDtypeStruct((3, count, wide), BF16),
                   jax.ShapeDtypeStruct((2, rows, columns), F32)),
        in_specs=[VMEM] * 4 + [pl.BlockSpec(memory_space=pl.ANY)] * 2,
        out_specs=(VMEM,) * 4,
        scratch_shapes=[
            pltpu.VMEM(w_up.shape, BF16), pltpu.VMEM(w_down.shape, BF16),
            pltpu.VMEM((rows, 128), F32), pltpu.VMEM((C - 1, rows, 128), F32),
            pltpu.VMEM((3, tokens, wide), BF16),
            pltpu.VMEM((3, 6, tokens, half), BF16), pltpu.VMEM((3, 6, tokens, half), BF16),
            pltpu.VMEM((3, 6, 1, half), F32), pltpu.VMEM((3, 6, 1, half), F32),
            pltpu.VMEM((3, 2, tokens, half), F32), pltpu.VMEM((3, 2, tokens, half), F32),
            pltpu.VMEM((2, chips, 2, rows, columns), F32),
            pltpu.VMEM((2, chips, rows, columns), F32),
            pltpu.VMEM((2, chips, rows, columns), BF16), pltpu.VMEM((2, chips, rows, columns), BF16),
            pltpu.VMEM((2, chips, 1, columns), F32), pltpu.VMEM((2, chips, 1, columns), F32),
        ]
        + [DMA((2,)), DMA((C - 1,)), DMA((C - 1,)),
           DMA((3, slots)), DMA((3, slots)), DMA((3, slots)), DMA((3, R)),
           DMA((3, 6)), DMA((3, 6)), DMA((3, 6)), DMA((3, 6)), DMA((3, 4)), DMA((3, 4))]
        + [DMA((2, chips))] * 6,
        compiler_params=pltpu.CompilerParams(
            collective_id=0, has_side_effects=True, vmem_limit_bytes=GRANT),
        cost_estimate=pl.CostEstimate(flops=10**10, bytes_accessed=10**7, transcendentals=0),
    )(x_fwd, x_bwd, grad_out, gain, w_up, w_down)


def final_kernel(R, C, width, gn, xb, go, gain, stats, squares, dx, g_gain, total,
                 st_own, st_in, gp_own, gp_in, tt_own, tt_in,
                 st_s, st_r, gp_s, gp_r, tt_s, tt_r):
    row, col = lax.axis_index("row"), lax.axis_index("col")
    cols = [{"row": row, "col": (col + i) % C} for i in range(1, C)]
    rows = [{"row": (row + i) % R, "col": col} for i in range(1, R)]
    greet(cols + rows)
    hat, inv = normal_of(xb[...].astype(F32), stats[...], 2, width)
    grad = gn[...]
    scaled = grad * gain[...]
    st_own[...] = lanes_of([jnp.sum(scaled, 1, keepdims=True), jnp.sum(scaled * hat, 1, keepdims=True)])
    first = [send(st_own, st_in.at[i], st_s.at[i], st_r.at[i], p) for i, p in enumerate(cols)]
    for copy in first:
        copy.start()
    wide = grad.shape[1]
    gp_own[:, :wide] = jnp.broadcast_to(jnp.sum(grad * hat, 0, keepdims=True), (8, wide))
    gp_own[:, wide:] = squares[...]
    gp_in[row] = gp_own[...]
    second = [send(gp_own, gp_in.at[row], gp_s.at[i], gp_r.at[i], p) for i, p in enumerate(rows)]
    for copy in second:
        copy.start()
    for copy in second:
        copy.wait()
    gains = gp_in[0]
    for i in range(1, R):
        gains = gains + gp_in[i]
    gained = gains[:, :wide]
    g_gain[...] = gained
    tt_own[...] = gains[:, wide:] + jnp.sum(gained * gained, 1, keepdims=True)
    tt_in[col] = tt_own[...]
    third = [send(tt_own, tt_in.at[col], tt_s.at[i], tt_r.at[i], p) for i, p in enumerate(cols)]
    for copy in third:
        copy.start()
    for copy in first:
        copy.wait()
    sums = st_own[...]
    for i in range(C - 1):
        sums = sums + st_in[i]
    c1, c2 = sums[:, 0:1] / width, sums[:, 1:2] / width
    dx[...] = (go[...].astype(F32) + inv * (scaled - c1 - hat * c2)).astype(BF16)
    for copy in third:
        copy.wait()
    whole = tt_in[0]
    for i in range(1, C):
        whole = whole + tt_in[i]
    total[...] = whole


def final(R, C, width, gn, x_bwd, grad_out, gain, stats, squares):
    rows, wide = gn.shape
    return pl.pallas_call(
        functools.partial(final_kernel, R, C, width),
        out_shape=(jax.ShapeDtypeStruct((rows, wide), BF16),
                   jax.ShapeDtypeStruct((8, wide), F32),
                   jax.ShapeDtypeStruct((8, 128), F32)),
        in_specs=[VMEM] * 6,
        out_specs=(VMEM, VMEM, VMEM),
        scratch_shapes=[
            pltpu.VMEM((rows, 128), F32), pltpu.VMEM((C - 1, rows, 128), F32),
            pltpu.VMEM((8, wide + 128), F32), pltpu.VMEM((R, 8, wide + 128), F32),
            pltpu.VMEM((8, 128), F32), pltpu.VMEM((C, 8, 128), F32),
            DMA((C - 1,)), DMA((C - 1,)), DMA((R - 1,)), DMA((R - 1,)), DMA((C - 1,)), DMA((C - 1,)),
        ],
        compiler_params=pltpu.CompilerParams(
            collective_id=3, has_side_effects=True, vmem_limit_bytes=GRANT),
        cost_estimate=pl.CostEstimate(flops=10**9, bytes_accessed=10**7, transcendentals=0),
    )(gn, x_bwd, grad_out, gain, stats, squares)


def with_kernels(R, C):
    def step(x_fwd, x_bwd, grad_out, gain, w_up, w_down):
        rows, columns = x_fwd.shape
        width = columns * C
        gain_row = gain.reshape(1, columns)
        full, stats, acts, sums = layer(R, C, width, x_fwd, x_bwd, grad_out, gain_row, w_up, w_down)
        y_fwd = (x_fwd.astype(F32) + sums[0]).astype(BF16)
        down_total = contract(acts[1], full[2], 0, 0)
        up_total = contract(full[1], acts[2], 0, 0)
        squares = jnp.sum(up_total * up_total) + jnp.sum(down_total * down_total)
        dx, g_gain, total = final(R, C, width, sums[1], x_bwd, grad_out, gain_row, stats,
                                  jnp.broadcast_to(squares, (8, 128)))
        param_count = 2 * width * w_up.shape[1] * R + width
        norm_value = jnp.sqrt(total[0, 0])
        grad_rms = norm_value / math.sqrt(param_count)
        factor = jnp.minimum(1.0, clip_share * math.sqrt(param_count) / norm_value)
        return (y_fwd, dx, up_total * factor, down_total * factor, g_gain[0] * factor, grad_rms)

    return step


def solution(mesh):
    placed = (
        P("row", "col"),
        P("row", "col"),
        P("row", "col"),
        P("col"),
        P("col", "row"),
        P("row", "col"),
    )
    R, C = mesh.shape["row"], mesh.shape["col"]
    body = with_kernels(R, C) if C == 4 and R % 2 == 0 else on_device
    return jax.shard_map(
        body,
        mesh=mesh,
        in_specs=placed,
        out_specs=(
            P("row", "col"),
            P("row", "col"),
            P("col", "row"),
            P("row", "col"),
            P("col"),
            P(),
        ),
        check_vma=False,
    )
```

```python
import functools
import math

import jax
import jax.numpy as jnp
from jax import lax
from jax.experimental import pallas as pl
from jax.experimental.pallas import tpu as pltpu
from jax.sharding import PartitionSpec as P

D = 6144
FF = 12288


eps = 1e-06
clip_share = 0.25


def erf_gelu(value):
    return 0.5 * value * (1.0 + lax.erf(value * 0.7071067811865476))


def gelu_slope(value):
    return (
        0.5 * (1.0 + lax.erf(value * 0.7071067811865476))
        + value * jnp.exp(-0.5 * value * value) * 0.3989422804014327
    )


def contract(left, right, left_dim, right_dim):
    return lax.dot_general(
        left, right, (((left_dim,), (right_dim,)), ((), ())), preferred_element_type=jnp.float32
    )


def row_sums(tokens):
    values = tokens.astype(jnp.float32)
    return (jnp.sum(values, -1), jnp.sum(values * values, -1))


def normalize(tokens, first, second):
    values = tokens.astype(jnp.float32)
    centre = first / D
    spread = second / D - centre * centre
    inv_scale = lax.rsqrt(spread + eps)
    return ((values - centre[:, None]) * inv_scale[:, None], inv_scale)


def up_both(normed_a, normed_b, w_up):
    full_a, full_b = (
        lax.all_gather(normed_a, "row", axis=0, tiled=True),
        lax.all_gather(normed_b, "row", axis=0, tiled=True),
    )
    width = w_up.shape[1]
    summed = lax.psum_scatter(
        jnp.concatenate(
            [
                jnp.dot(full_a, w_up, preferred_element_type=jnp.float32),
                jnp.dot(full_b, w_up, preferred_element_type=jnp.float32),
            ],
            1,
        ),
        "col",
        scatter_dimension=0,
        tiled=True,
    )
    return (summed[:, :width], summed[:, width:], full_b)


def on_device(x_fwd, x_bwd, grad_out, gain, w_up, w_down):
    first_a, second_a = row_sums(x_fwd)
    first_b, second_b = row_sums(x_bwd)
    first_a, second_a, first_b, second_b = lax.psum((first_a, second_a, first_b, second_b), "col")
    centred_a, _ = normalize(x_fwd, first_a, second_a)
    centred_b, inv_scale = normalize(x_bwd, first_b, second_b)
    normed_a = (centred_a * gain).astype(jnp.bfloat16)
    normed_b = (centred_b * gain).astype(jnp.bfloat16)
    pre_a, pre_b, normed_full = up_both(normed_a, normed_b, w_up)
    hidden_a = erf_gelu(pre_a).astype(jnp.bfloat16)
    output_part = jnp.dot(
        lax.all_gather(hidden_a, "col", axis=0, tiled=True),
        w_down,
        preferred_element_type=jnp.float32,
    )
    output_sum = lax.psum_scatter(output_part, "row", scatter_dimension=0, tiled=True)
    y_fwd = (x_fwd.astype(jnp.float32) + output_sum).astype(jnp.bfloat16)
    hidden_b = erf_gelu(pre_b).astype(jnp.bfloat16)
    grad_full = lax.all_gather(grad_out, "row", axis=0, tiled=True)
    grad_hidden = lax.psum_scatter(
        contract(grad_full, w_down, 1, 1), "col", scatter_dimension=0, tiled=True
    )
    grad_pre = (grad_hidden * gelu_slope(pre_b)).astype(jnp.bfloat16)
    hidden_piece = lax.all_gather(hidden_b, "col", axis=0, tiled=True)
    pre_piece = lax.all_gather(grad_pre, "col", axis=0, tiled=True)
    down_total = contract(hidden_piece, grad_full, 0, 0)
    up_total = contract(normed_full, pre_piece, 0, 0)
    input_total = contract(pre_piece, w_up, 1, 1)
    grad_normed = lax.psum_scatter(input_total, "row", scatter_dimension=0, tiled=True)
    scaled = grad_normed * gain
    first_back = jnp.sum(scaled, -1)
    second_back = jnp.sum(scaled * centred_b, -1)
    first_back, second_back = lax.psum((first_back, second_back), "col")
    dx_bwd = (
        grad_out.astype(jnp.float32)
        + inv_scale[:, None]
        * (scaled - first_back[:, None] / D - centred_b * (second_back[:, None] / D))
    ).astype(jnp.bfloat16)
    gain_part = jnp.sum(grad_normed * centred_b, 0)
    weight_squares = jnp.sum(up_total * up_total) + jnp.sum(down_total * down_total)
    g_gain = lax.psum(gain_part, "row")
    first_row = (lax.axis_index("row") == 0).astype(jnp.float32)
    total = lax.psum(weight_squares + first_row * jnp.sum(g_gain * g_gain), ("row", "col"))
    param_count = 2 * D * FF + D
    norm_value = jnp.sqrt(total)
    grad_rms = norm_value / math.sqrt(param_count)
    factor = jnp.minimum(1.0, clip_share * math.sqrt(param_count) / norm_value)
    return (y_fwd, dx_bwd, up_total * factor, down_total * factor, g_gain * factor, grad_rms)


MESH = pl.DeviceIdType.MESH
VMEM = pl.BlockSpec(memory_space=pltpu.VMEM)
F32 = jnp.float32
BF16 = jnp.bfloat16
DMA = pltpu.SemaphoreType.DMA
GRANT = 45 * 1024 * 1024


def send(src, dst, send_sem, recv_sem, peer):
    return pltpu.make_async_remote_copy(
        src_ref=src, dst_ref=dst, send_sem=send_sem, recv_sem=recv_sem,
        device_id=peer, device_id_type=MESH,
    )


def arrived(ref, sem, peer):
    pltpu.make_async_remote_copy(
        src_ref=ref, dst_ref=ref, send_sem=sem, recv_sem=sem,
        device_id=peer, device_id_type=MESH,
    ).wait_recv()


SPAN = 252.0


def encode(values):
    size = jnp.abs(values)
    peak = jnp.maximum(jnp.max(size, 0, keepdims=True), 1e-30)
    code = jnp.exp2(size * (SPAN / peak) - 0.5 * SPAN)
    return jnp.where(values < 0.0, -code, code).astype(BF16), peak


def decode(codes, peak):
    code = codes.astype(F32)
    size = jnp.log(jnp.abs(code)) * (peak * (1.4426950408889634 / SPAN)) + 0.5 * peak
    return jnp.where(code < 0.0, -size, size)


def normal_of(values, stats, at, width):
    centre = stats[:, at : at + 1] / width
    spread = stats[:, at + 1 : at + 2] / width - centre * centre
    inv = lax.rsqrt(spread + eps)
    return (values - centre) * inv, inv


def lanes_of(columns):
    rows = columns[0].shape[0]
    lane = lax.broadcasted_iota(jnp.int32, (rows, 128), 1)
    out = jnp.zeros((rows, 128), F32)
    for i, column in enumerate(columns):
        out = jnp.where(lane == i, column, out)
    return out


def step_kernel(R, C, width, params, xa, xb, go, gain, w_up_hbm, w_down_hbm,
                g_up, g_down, y, dx, gained, verdict,
                full, acts, w_up, w_down, gain_row, st_own, st_in, keep, buf, inb, buf_p, inb_p,
                part, from_sib, zbuf, zin, zbuf_p, zin_p, mine, sq,
                back_own, back_in, gp_own, gp_in, tt_own, tt_in, uu_own, uu_in,
                w_sem, st_s, st_r, s_right, s_left, s_sib, recv, hop_s, hop_r, peak_s, peak_r,
                g_s, g_r, sib_s, sib_r, z_s, z_r, zp_s, zp_r,
                back_s, back_r, gp_s, gp_r, tt_s, tt_r, uu_s, uu_r):
    row, col = lax.axis_index("row"), lax.axis_index("col")
    chips = R // 2
    chip, core = row // 2, row % 2
    sib = {"row": row + 1 - 2 * core, "col": col}
    cols = [{"row": row, "col": (col + i) % C} for i in range(1, C)]
    rows_of = [{"row": (row + i) % R, "col": col} for i in range(1, R)]
    flip_x = col + 1 - 2 * (col % 2)
    flip_y = (col + 2) % 4
    diag = 3 - col
    peer_x, peer_y = {"row": row, "col": flip_x}, {"row": row, "col": flip_y}
    share, columns = xa.shape
    tokens = share * R // C
    wide = w_up.shape[1]
    half = wide // 2
    tile = half // 2
    high = chip // 2

    def line(step):
        return {"row": row + 2 * step, "col": col}

    def mirror(at, on):
        return at + on * (chips - 1 - 2 * at)

    def order(k):
        low = mirror(chip, high)
        return mirror((low, 1 - low, 2, 3)[k], high)

    load_up = pltpu.make_async_copy(w_up_hbm, w_up, w_sem.at[0])
    load_down = pltpu.make_async_copy(w_down_hbm, w_down, w_sem.at[1])
    load_down.start()
    load_up.start()
    barrier = pltpu.get_barrier_semaphore()
    for peer in cols + rows_of:
        pl.semaphore_signal(barrier, inc=1, device_id=peer, device_id_type=MESH)
    moments = []
    for x in (xa, xb):
        v = x[...].astype(F32)
        moments += [jnp.sum(v, 1, keepdims=True), jnp.sum(v * v, 1, keepdims=True)]
    st_own[...] = lanes_of(moments)
    for i in range(columns // 128):
        gain_row[:, i * 128 : (i + 1) * 128] = gain[i : i + 1, :]
    sq[...] = jnp.zeros_like(sq)
    pl.semaphore_wait(barrier, len(cols) + len(rows_of))

    def block(j, owner):
        return full.at[j, pl.ds(owner * share, share), :]

    def spread(j, owner, slot, src, to_right, to_left):
        dst = block(j, owner)
        out = [(None, send(src, dst, s_sib.at[j, slot], recv.at[j, owner], sib))]
        if to_right:
            out.append((chip < chips - 1,
                        send(src, dst, s_right.at[j, slot], recv.at[j, owner], line(1))))
        if to_left:
            out.append((chip > 0,
                        send(src, dst, s_left.at[j, slot], recv.at[j, owner], line(-1))))
        return out

    def start(copies):
        for cond, copy in copies[::-1]:
            if cond is None:
                copy.start()
            else:
                pl.when(cond)(copy.start)

    def finish(copies):
        for cond, copy in copies:
            if cond is None:
                copy.wait_send()
            else:
                pl.when(cond)(copy.wait_send)

    mine_of = {2: spread(2, row, 0, go, True, True)}
    start(mine_of[2])
    st_copies = [send(st_own, st_in.at[i], st_s.at[i], st_r.at[i], p) for i, p in enumerate(cols)]
    for copy in st_copies:
        copy.start()
    block(2, row)[...] = go[...]

    def relays(j, visit, steps):
        for step in steps:
            for sign in (-1, 1):
                ok = chip >= step if sign < 0 else chip + step < chips

                @pl.when(ok)
                def _():
                    owner = row + 2 * sign * step
                    slot = step if sign < 0 else chips - 1 + step
                    visit(owner, sign, spread(j, owner, slot, block(j, owner), sign < 0, sign > 0))

    def gather(j, step):
        def visit(owner, sign, copies):
            arrived(block(j, owner), recv.at[j, owner], line(sign))
            start(copies)

        relays(j, visit, (step,))

    ends = (chip + 1) % chips < 2

    def gather_for(j, k):
        if k == 1:
            gather(j, 1)
        elif k == 2:
            pl.when(ends)(lambda: gather(j, 2))
        elif k == 3:
            pl.when(jnp.logical_not(ends))(lambda: gather(j, 2))
            pl.when(ends)(lambda: gather(j, 3))

    def hop(j, s, peer):
        return (send(buf.at[j, s], inb.at[j, s], hop_s.at[j, s], hop_r.at[j, s], peer),
                send(buf_p.at[j, s], inb_p.at[j, s], peak_s.at[j, s], peak_r.at[j, s], peer))

    def go_hop(j, s, peer):
        for copy in hop(j, s, peer):
            copy.start()

    def got_hop(j, s):
        for copy in hop(j, s, peer_x):
            copy.wait_recv()

    def over_tiles(body, size):
        @pl.loop(0, size // tile)
        def _(t):
            body(pl.ds(pl.multiple_of(t * tile, tile), tile))

    def role_of(q):
        return (q + col) % 2, (q // 2 + col // 2) % 2

    def product(j, k):
        q = order(k)
        owner = 2 * q + 1 - core
        arrived(block(j, owner), recv.at[j, owner], sib)
        off_x, off_y = role_of(q)

        @pl.loop(0, 2)
        def _(h):
            now = off_x + h * (off_y - off_x)
            slot = 2 * (1 - off_y) + h * (1 - 2 * off_x + 2 * off_y)
            s = 2 * (1 - off_y) + h * (3 - 4 * off_x + 2 * off_y)
            at = pl.ds(pl.multiple_of(h * half, half), half)
            left = full[j, pl.ds(q * tokens, tokens), :]
            if j == 2:
                piece = lax.dot_general(left, w_down[at, :], (((1,), (1,)), ((), ())),
                                        preferred_element_type=F32)
            else:
                piece = jnp.dot(left, w_up[:, at], preferred_element_type=F32)
            place = now * 12 + (1 - now) * (j * 4 + slot)
            keep[place] = piece

            @pl.when(now == 1)
            def _():
                def code(part_of):
                    buf[j, s, :, part_of], buf_p[j, s, :, part_of] = encode(keep[12, :, part_of])

                over_tiles(code, half)
                go_hop(j, s, {"row": row, "col": flip_x + h * (flip_y - flip_x)})

    def merge(j, k):
        off_x, off_y = role_of(order(k))

        @pl.when(off_x + off_y == 1)
        def _():
            got_hop(j, off_x)

            def add(at):
                merged = keep[j * 4 + off_x, :, at] + decode(inb[j, off_x, :, at], inb_p[j, off_x, :, at])
                buf[j, 4 - off_x, :, at], buf_p[j, 4 - off_x, :, at] = encode(merged)

            over_tiles(add, half)
            go_hop(j, 4 - off_x, {"row": row, "col": flip_y + off_x * (flip_x - flip_y)})

    def landed(j):
        for s in range(2, 6):
            got_hop(j, s)

    def summed(j, h, at):
        return (keep[j * 4 + 2 + h, at, :] + decode(inb[j, 2 + h, at, :], inb_p[j, 2 + h])
                + decode(inb[j, 4 + h, at, :], inb_p[j, 4 + h]))

    chunk = 16

    def over(body):
        @pl.loop(0, tokens // chunk)
        def _(i):
            at = pl.ds(pl.multiple_of(i * chunk, chunk), chunk)
            to = pl.ds(pl.multiple_of(col * tokens + i * chunk, chunk), chunk)
            for h in range(2):
                body(h, at, to, slice(h * half, (h + 1) * half))

    def backward(h, at, to, across):
        v = summed(1, h, at)
        phi = 0.5 * (1.0 + lax.erf(v * 0.7071067811865476))
        g = summed(2, h, at)
        slope = phi + v * jnp.exp(-0.5 * v * v) * 0.3989422804014327
        acts[1, to, across] = (v * phi).astype(BF16)
        acts[2, to, across] = (g * slope).astype(BF16)

    def forward(h, at, to, across):
        v = summed(0, h, at)
        acts[0, to, across] = (0.5 * v * (1.0 + lax.erf(v * 0.7071067811865476))).astype(BF16)

    def piece_of(k, owner, h):
        return acts.at[k, pl.ds(pl.multiple_of(owner * tokens, tokens), tokens), pl.ds(h * half, half)]

    def passing(k, i):
        owner, h, peer = ((col, 0, peer_x), (col, 1, peer_y), (col, 1, peer_x), (col, 0, peer_y),
                          (flip_x, 0, peer_y), (flip_y, 1, peer_x))[i]
        ref = piece_of(k, owner, h)
        return send(ref, ref, g_s.at[k, i], g_r.at[k, i], peer)

    def publish(k):
        for i in range(4):
            passing(k, i).start()

    def pass_on(k):
        arrived(piece_of(k, flip_x, 0), g_r.at[k, 0], peer_x)
        passing(k, 4).start()
        arrived(piece_of(k, flip_y, 1), g_r.at[k, 1], peer_y)
        passing(k, 5).start()

    def sides(k):
        arrived(piece_of(k, flip_x, 1), g_r.at[k, 2], peer_x)
        arrived(piece_of(k, flip_y, 0), g_r.at[k, 3], peer_y)

    def corner(k):
        arrived(piece_of(k, diag, 0), g_r.at[k, 4], peer_y)
        arrived(piece_of(k, diag, 1), g_r.at[k, 5], peer_x)

    roles = (col, flip_x, flip_y, diag)

    def to_sib(j, i):
        return send(part.at[j, i, 1 - core], from_sib.at[j, i], sib_s.at[j, i], sib_r.at[j, i], sib)

    def to_owner(j, i):
        peer = {"row": 2 * roles[i] + core, "col": col}
        return (send(zbuf.at[j, i], zin.at[j, chip], z_s.at[j, i], z_r.at[j, chip], peer),
                send(zbuf_p.at[j, i], zin_p.at[j, chip], zp_s.at[j, i], zp_r.at[j, chip], peer))

    def second(j, i):
        @pl.loop(0, 2)
        def _(h):
            at = pl.ds(pl.multiple_of(h * half, half), half)
            left = acts[2 * j, pl.ds(pl.multiple_of(roles[i] * tokens, tokens), tokens), :]
            if j == 0:
                piece = jnp.dot(left, w_down[:, at], preferred_element_type=F32)
            else:
                piece = lax.dot_general(left, w_up[at, :], (((1,), (1,)), ((), ())),
                                        preferred_element_type=F32)
            part[j, i, 0, :, at] = piece[:share]
            part[j, i, 1, :, at] = piece[share:]

        to_sib(j, i).start()

    def onward(j, i):
        to_sib(j, i).wait_recv()
        away = roles[i] != chip

        @pl.when(away)
        def _():
            def code(at):
                zbuf[j, i, :, at], zbuf_p[j, i, :, at] = encode(
                    part[j, i, core, :, at] + from_sib[j, i, :, at])

            over_tiles(code, columns)
            for copy in to_owner(j, i):
                copy.start()

        @pl.when(jnp.logical_not(away))
        def _():
            mine[j] = part[j, i, core] + from_sib[j, i]

    def collect(j):
        for z in range(chips):
            @pl.when(z != chip)
            def _():
                peer = {"row": 2 * z + core, "col": col}
                arrived(zin.at[j, z], z_r.at[j, z], peer)
                arrived(zin_p.at[j, z], zp_r.at[j, z], peer)
                mine[j] = mine[j] + decode(zin[j, z], zin_p[j, z])

    def gradient(out, left, right):
        step_m, step_n = 256, half

        @pl.loop(0, out.shape[0] // step_m)
        def _(m):
            at = pl.ds(pl.multiple_of(m * step_m, step_m), step_m)
            for n in range(out.shape[1] // step_n):
                across = slice(n * step_n, (n + 1) * step_n)
                piece = lax.dot_general(left[:, at], right[:, across], (((0,), (0,)), ((), ())),
                                        preferred_element_type=F32)
                out[at, across] = piece
                sq[:, across] = sq[:, across] + jnp.sum(piece * piece, 0, keepdims=True)

    load_down.wait()
    product(2, 0)
    gather_for(2, 1)
    for copy in st_copies:
        copy.wait()
    stats = st_own[...]
    for i in range(C - 1):
        stats = stats + st_in[i]
    for j, x, at in ((1, xb, 2), (0, xa, 0)):
        hat, _ = normal_of(x[...].astype(F32), stats, at, width)
        block(j, row)[...] = (hat * gain_row[...]).astype(BF16)
        mine_of[j] = spread(j, row, 0, block(j, row), True, True)
        if j == 1:
            start(mine_of[1])
    product(2, 1)
    merge(2, 0)
    gather_for(2, 2)
    product(2, 2)
    merge(2, 1)
    gather_for(2, 3)
    start(mine_of[0])
    load_up.wait()
    product(2, 3)
    merge(2, 2)
    product(1, 0)
    gather_for(1, 1)
    merge(2, 3)
    product(1, 1)
    merge(1, 0)
    gather_for(1, 2)
    product(1, 2)
    merge(1, 1)
    gather_for(1, 3)
    product(1, 3)
    merge(1, 2)
    product(0, 0)
    gather_for(0, 1)
    merge(1, 3)
    landed(2)
    landed(1)
    over(backward)
    publish(2)
    publish(1)
    product(0, 1)
    merge(0, 0)
    second(1, 0)
    gather_for(0, 2)
    product(0, 2)
    merge(0, 1)
    pass_on(2)
    gather_for(0, 3)
    product(0, 3)
    merge(0, 2)
    onward(1, 0)
    sides(2)
    second(1, 1)
    merge(0, 3)
    second(1, 2)
    pass_on(1)
    landed(0)
    over(forward)
    publish(0)
    onward(1, 1)
    onward(1, 2)
    corner(2)
    second(1, 3)
    second(0, 0)
    onward(1, 3)
    gradient(g_up, full.at[1], acts.at[2])
    onward(0, 0)
    sides(1)
    corner(1)
    pass_on(0)
    gradient(g_down, acts.at[1], full.at[2])
    tt_own[...] = jnp.broadcast_to(jnp.sum(sq[...], 1, keepdims=True), tt_own.shape)
    third = [send(tt_own, tt_in.at[row], tt_s.at[i], tt_r.at[i], p) for i, p in enumerate(rows_of)]
    for copy in third:
        copy.start()
    sides(0)
    second(0, 1)
    second(0, 2)
    collect(1)
    grad = mine[1]
    hat, inv = normal_of(xb[...].astype(F32), stats, 2, width)
    scaled = grad * gain_row[...]
    back_own[...] = lanes_of([jnp.sum(scaled, 1, keepdims=True), jnp.sum(scaled * hat, 1, keepdims=True)])
    first = [send(back_own, back_in.at[i], back_s.at[i], back_r.at[i], p) for i, p in enumerate(cols)]
    for copy in first:
        copy.start()
    gain_part = jnp.sum(grad * hat, 0, keepdims=True)
    for i in range(columns // 128):
        gp_own[i : i + 1, :] = gain_part[:, i * 128 : (i + 1) * 128]
    gains_out = [send(gp_own, gp_in.at[row], gp_s.at[i], gp_r.at[i], p) for i, p in enumerate(rows_of)]
    for copy in gains_out:
        copy.start()
    onward(0, 1)
    onward(0, 2)
    corner(0)
    second(0, 3)
    gp_in[row] = gp_own[...]
    tt_in[row] = tt_own[...]
    for copy in gains_out + third:
        copy.wait()
    onward(0, 3)
    gains, squares = gp_in[0], tt_in[0]
    for i in range(1, R):
        gains, squares = gains + gp_in[i], squares + tt_in[i]
    gained[...] = gains
    uu_own[...] = squares + jnp.sum(gains * gains)
    fourth = [send(uu_own, uu_in.at[col], uu_s.at[i], uu_r.at[i], p) for i, p in enumerate(cols)]
    for copy in fourth:
        copy.start()
    uu_in[col] = uu_own[...]
    for copy in first:
        copy.wait()
    sums = back_own[...]
    for i in range(C - 1):
        sums = sums + back_in[i]
    c1, c2 = sums[:, 0:1] / width, sums[:, 1:2] / width
    hat, inv = normal_of(xb[...].astype(F32), stats, 2, width)
    scaled = mine[1] * gain_row[...]
    dx[...] = (go[...].astype(F32) + inv * (scaled - c1 - hat * c2)).astype(BF16)
    for copy in fourth:
        copy.wait()
    total = uu_in[0]
    for i in range(1, C):
        total = total + uu_in[i]
    norm_value = jnp.sqrt(total)
    verdict[0] = jnp.minimum(1.0, clip_share * math.sqrt(params) / norm_value)
    verdict[1] = norm_value / math.sqrt(params)
    collect(0)
    y[...] = (xa[...].astype(F32) + mine[0]).astype(BF16)

    for j in (2, 1, 0):
        finish(mine_of[j])
        relays(j, lambda owner, sign, copies: finish(copies), range(1, chips))
        for i in range(6):
            passing(j, i).wait_send()
            for copy in hop(j, i, peer_x):
                copy.wait_send()
    for j in (0, 1):
        for i in range(chips):
            to_sib(j, i).wait_send()

            @pl.when(roles[i] != chip)
            def _():
                for copy in to_owner(j, i):
                    copy.wait_send()


def step_on_core(R, C, width, params, x_fwd, x_bwd, grad_out, gain, w_up, w_down):
    rows, columns = x_fwd.shape
    wide = w_up.shape[1]
    chips, slots = R // 2, 2 * (R // 2) - 1
    count = rows * R
    tokens, half = count // C, wide // 2
    lines = columns // 128
    VM = pltpu.VMEM
    return pl.pallas_call(
        functools.partial(step_kernel, R, C, width, params),
        out_shape=(VM((columns, wide), F32), VM((wide, columns), F32), VM((rows, columns), BF16),
                   VM((rows, columns), BF16), VM((lines, 128), F32), VM((2, 8, 128), F32)),
        in_specs=[VMEM] * 4 + [pl.BlockSpec(memory_space=pl.ANY)] * 2,
        out_specs=(VMEM,) * 6,
        scratch_shapes=[
            VM((3, count, columns), BF16), VM((3, count, wide), BF16),
            VM(w_up.shape, BF16), VM(w_down.shape, BF16), VM((1, columns), F32),
            VM((rows, 128), F32), VM((C - 1, rows, 128), F32),
            VM((13, tokens, half), F32),
            VM((3, 6, tokens, half), BF16), VM((3, 6, tokens, half), BF16),
            VM((3, 6, 1, half), F32), VM((3, 6, 1, half), F32),
            VM((2, chips, 2, rows, columns), F32), VM((2, chips, rows, columns), F32),
            VM((2, chips, rows, columns), BF16), VM((2, chips, rows, columns), BF16),
            VM((2, chips, 1, columns), F32), VM((2, chips, 1, columns), F32),
            VM((2, rows, columns), F32), VM((1, columns), F32),
            VM((rows, 128), F32), VM((C - 1, rows, 128), F32),
            VM((lines, 128), F32), VM((R, lines, 128), F32),
            VM((8, 128), F32), VM((R, 8, 128), F32), VM((8, 128), F32), VM((C, 8, 128), F32),
        ]
        + [DMA((2,)), DMA((C - 1,)), DMA((C - 1,)),
           DMA((3, slots)), DMA((3, slots)), DMA((3, slots)), DMA((3, R))]
        + [DMA((3, 6))] * 6 + [DMA((2, chips))] * 6
        + [DMA((C - 1,))] * 2 + [DMA((R - 1,))] * 4 + [DMA((C - 1,))] * 2,
        compiler_params=pltpu.CompilerParams(
            collective_id=0, has_side_effects=True, vmem_limit_bytes=GRANT),
        cost_estimate=pl.CostEstimate(flops=2 * 10**10, bytes_accessed=10**7, transcendentals=0),
    )(x_fwd, x_bwd, grad_out, gain, w_up, w_down)


def clip_kernel(g_up, g_down, y_in, dx_in, gains, verdict, up, down, y, dx, step_gain, rms, staged, sem):
    factor = verdict[0, 0:1, 0:1]
    slots = staged.shape[1]
    size = staged.shape[2]
    for which, (grad, out) in enumerate(((g_up, up), (g_down, down))):
        for i in range(slots):
            at = pl.ds(i * size, size)
            staged[which, i] = grad[at, :] * factor
            pltpu.make_async_copy(staged.at[which, i], out.at[at, :], sem.at[which, i]).start()
    y[...] = y_in[...]
    dx[...] = dx_in[...]
    step_gain[...] = gains[...] * factor
    rms[...] = verdict[1, 0:1, 0:1]
    for which, out in enumerate((up, down)):
        for i in range(slots):
            at = pl.ds(i * size, size)
            pltpu.make_async_copy(staged.at[which, i], out.at[at, :], sem.at[which, i]).wait()


def clip(g_up, g_down, y, dx, gains, verdict):
    slots = 12
    size = g_up.shape[0] // slots
    like = jax.ShapeDtypeStruct
    return pl.pallas_call(
        clip_kernel,
        out_shape=(like(g_up.shape, F32), like(g_down.shape, F32), like(y.shape, BF16),
                   like(dx.shape, BF16), like(gains.shape, F32), like((1, 1), F32)),
        in_specs=[VMEM] * 6,
        out_specs=(pl.BlockSpec(memory_space=pl.ANY),) * 2 + (VMEM,) * 4,
        scratch_shapes=[pltpu.VMEM((2, slots, size, g_up.shape[1]), F32), DMA((2, slots))],
        compiler_params=pltpu.CompilerParams(vmem_limit_bytes=40 * 1024 * 1024),
        cost_estimate=pl.CostEstimate(flops=10**8, bytes_accessed=4 * 10**7, transcendentals=0),
    )(g_up, g_down, y, dx, gains, verdict)


def with_kernels(R, C):
    def step(x_fwd, x_bwd, grad_out, gain, w_up, w_down):
        rows, columns = x_fwd.shape
        width = columns * C
        params = 2 * width * w_up.shape[1] * R + width
        parts = step_on_core(R, C, width, params, x_fwd, x_bwd, grad_out,
                             gain.reshape(columns // 128, 128), w_up, w_down)
        up, down, y, dx, step_gain, rms = clip(*parts)
        return y, dx, up, down, step_gain.reshape(columns), rms.reshape(())

    return step


def solution(mesh):
    placed = (
        P("row", "col"),
        P("row", "col"),
        P("row", "col"),
        P("col"),
        P("col", "row"),
        P("row", "col"),
    )
    R, C = mesh.shape["row"], mesh.shape["col"]
    body = with_kernels(R, C) if C == 4 and R == 8 else on_device
    return jax.shard_map(
        body,
        mesh=mesh,
        in_specs=placed,
        out_specs=(
            P("row", "col"),
            P("row", "col"),
            P("col", "row"),
            P("row", "col"),
            P("col"),
            P(),
        ),
        check_vma=False,
    )
```

```python
import functools
import math

import jax
import jax.numpy as jnp
from jax import lax
from jax.experimental import pallas as pl
from jax.experimental.pallas import tpu as pltpu
from jax.sharding import PartitionSpec as P

D = 6144
FF = 12288


eps = 1e-06
clip_share = 0.25


def erf_gelu(value):
    return 0.5 * value * (1.0 + lax.erf(value * 0.7071067811865476))


def gelu_slope(value):
    return (
        0.5 * (1.0 + lax.erf(value * 0.7071067811865476))
        + value * jnp.exp(-0.5 * value * value) * 0.3989422804014327
    )


def contract(left, right, left_dim, right_dim):
    return lax.dot_general(
        left, right, (((left_dim,), (right_dim,)), ((), ())), preferred_element_type=jnp.float32
    )


def row_sums(tokens):
    values = tokens.astype(jnp.float32)
    return (jnp.sum(values, -1), jnp.sum(values * values, -1))


def normalize(tokens, first, second):
    values = tokens.astype(jnp.float32)
    centre = first / D
    spread = second / D - centre * centre
    inv_scale = lax.rsqrt(spread + eps)
    return ((values - centre[:, None]) * inv_scale[:, None], inv_scale)


def up_both(normed_a, normed_b, w_up):
    full_a, full_b = (
        lax.all_gather(normed_a, "row", axis=0, tiled=True),
        lax.all_gather(normed_b, "row", axis=0, tiled=True),
    )
    width = w_up.shape[1]
    summed = lax.psum_scatter(
        jnp.concatenate(
            [
                jnp.dot(full_a, w_up, preferred_element_type=jnp.float32),
                jnp.dot(full_b, w_up, preferred_element_type=jnp.float32),
            ],
            1,
        ),
        "col",
        scatter_dimension=0,
        tiled=True,
    )
    return (summed[:, :width], summed[:, width:], full_b)


def on_device(x_fwd, x_bwd, grad_out, gain, w_up, w_down):
    first_a, second_a = row_sums(x_fwd)
    first_b, second_b = row_sums(x_bwd)
    first_a, second_a, first_b, second_b = lax.psum((first_a, second_a, first_b, second_b), "col")
    centred_a, _ = normalize(x_fwd, first_a, second_a)
    centred_b, inv_scale = normalize(x_bwd, first_b, second_b)
    normed_a = (centred_a * gain).astype(jnp.bfloat16)
    normed_b = (centred_b * gain).astype(jnp.bfloat16)
    pre_a, pre_b, normed_full = up_both(normed_a, normed_b, w_up)
    hidden_a = erf_gelu(pre_a).astype(jnp.bfloat16)
    output_part = jnp.dot(
        lax.all_gather(hidden_a, "col", axis=0, tiled=True),
        w_down,
        preferred_element_type=jnp.float32,
    )
    output_sum = lax.psum_scatter(output_part, "row", scatter_dimension=0, tiled=True)
    y_fwd = (x_fwd.astype(jnp.float32) + output_sum).astype(jnp.bfloat16)
    hidden_b = erf_gelu(pre_b).astype(jnp.bfloat16)
    grad_full = lax.all_gather(grad_out, "row", axis=0, tiled=True)
    grad_hidden = lax.psum_scatter(
        contract(grad_full, w_down, 1, 1), "col", scatter_dimension=0, tiled=True
    )
    grad_pre = (grad_hidden * gelu_slope(pre_b)).astype(jnp.bfloat16)
    hidden_piece = lax.all_gather(hidden_b, "col", axis=0, tiled=True)
    pre_piece = lax.all_gather(grad_pre, "col", axis=0, tiled=True)
    down_total = contract(hidden_piece, grad_full, 0, 0)
    up_total = contract(normed_full, pre_piece, 0, 0)
    input_total = contract(pre_piece, w_up, 1, 1)
    grad_normed = lax.psum_scatter(input_total, "row", scatter_dimension=0, tiled=True)
    scaled = grad_normed * gain
    first_back = jnp.sum(scaled, -1)
    second_back = jnp.sum(scaled * centred_b, -1)
    first_back, second_back = lax.psum((first_back, second_back), "col")
    dx_bwd = (
        grad_out.astype(jnp.float32)
        + inv_scale[:, None]
        * (scaled - first_back[:, None] / D - centred_b * (second_back[:, None] / D))
    ).astype(jnp.bfloat16)
    gain_part = jnp.sum(grad_normed * centred_b, 0)
    weight_squares = jnp.sum(up_total * up_total) + jnp.sum(down_total * down_total)
    g_gain = lax.psum(gain_part, "row")
    first_row = (lax.axis_index("row") == 0).astype(jnp.float32)
    total = lax.psum(weight_squares + first_row * jnp.sum(g_gain * g_gain), ("row", "col"))
    param_count = 2 * D * FF + D
    norm_value = jnp.sqrt(total)
    grad_rms = norm_value / math.sqrt(param_count)
    factor = jnp.minimum(1.0, clip_share * math.sqrt(param_count) / norm_value)
    return (y_fwd, dx_bwd, up_total * factor, down_total * factor, g_gain * factor, grad_rms)


MESH = pl.DeviceIdType.MESH
VMEM = pl.BlockSpec(memory_space=pltpu.VMEM)
F32 = jnp.float32
BF16 = jnp.bfloat16
DMA = pltpu.SemaphoreType.DMA
GRANT = 45 * 1024 * 1024


def send(src, dst, send_sem, recv_sem, peer):
    return pltpu.make_async_remote_copy(
        src_ref=src, dst_ref=dst, send_sem=send_sem, recv_sem=recv_sem,
        device_id=peer, device_id_type=MESH,
    )


def arrived(ref, sem, peer):
    pltpu.make_async_remote_copy(
        src_ref=ref, dst_ref=ref, send_sem=sem, recv_sem=sem,
        device_id=peer, device_id_type=MESH,
    ).wait_recv()


SPAN = 252.0


def encode(values):
    size = jnp.abs(values)
    peak = jnp.maximum(jnp.max(size, 0, keepdims=True), 1e-30)
    code = jnp.exp2(size * (SPAN / peak) - 0.5 * SPAN)
    return jnp.where(values < 0.0, -code, code).astype(BF16), peak


def decode(codes, peak):
    code = codes.astype(F32)
    size = jnp.log(jnp.abs(code)) * (peak * (1.4426950408889634 / SPAN)) + 0.5 * peak
    return jnp.where(code < 0.0, -size, size)


def normal_of(values, stats, at, width):
    centre = stats[:, at : at + 1] / width
    spread = stats[:, at + 1 : at + 2] / width - centre * centre
    inv = lax.rsqrt(spread + eps)
    return (values - centre) * inv, inv


def lanes_of(columns):
    rows = columns[0].shape[0]
    lane = lax.broadcasted_iota(jnp.int32, (rows, 128), 1)
    out = jnp.zeros((rows, 128), F32)
    for i, column in enumerate(columns):
        out = jnp.where(lane == i, column, out)
    return out


def step_kernel(R, C, width, params, xa, xb, go, gain, w_up_hbm, w_down_hbm,
                g_up, g_down, y, dx, gained, verdict,
                full, acts, w_up, w_down, gain_row, st_own, st_in, partial, buf, inb, buf_p, inb_p,
                part, from_sib, zbuf, zin, zmid, zbuf_p, zin_p, zmid_p, mine, sq,
                back_own, back_in, gp_own, gp_in, tt_own, tt_in, uu_own, uu_in,
                w_sem, st_s, st_r, s_right, s_left, s_sib, recv, hop_s, hop_r, peak_s, peak_r,
                g_s, g_r, sib_s, sib_r, z_s, z_r, zp_s, zp_r, zm_r, zmp_r,
                back_s, back_r, gp_s, gp_r, tt_s, tt_r, uu_s, uu_r):
    row, col = lax.axis_index("row"), lax.axis_index("col")
    chips = R // 2
    chip, core = row // 2, row % 2
    sib = {"row": row + 1 - 2 * core, "col": col}
    cols = [{"row": row, "col": (col + i) % C} for i in range(1, C)]
    rows_of = [{"row": (row + i) % R, "col": col} for i in range(1, R)]
    flip_x = col + 1 - 2 * (col % 2)
    flip_y = (col + 2) % 4
    diag = 3 - col
    peer_x, peer_y = {"row": row, "col": flip_x}, {"row": row, "col": flip_y}
    share, columns = xa.shape
    tokens = share * R // C
    wide = w_up.shape[1]
    half = wide // 2
    quarter = wide // C
    upper = tokens // 2
    tile = half // 2
    high = chip // 2

    def line(step):
        return {"row": row + 2 * step, "col": col}

    def mirror(at, on):
        return at + on * (chips - 1 - 2 * at)

    def order(k):
        low = mirror(chip, high)
        return mirror((low, 1 - low, 2, 3)[k], high)

    load_up = pltpu.make_async_copy(w_up_hbm, w_up, w_sem.at[0])
    load_down = pltpu.make_async_copy(w_down_hbm, w_down, w_sem.at[1])
    load_down.start()
    load_up.start()
    barrier = pltpu.get_barrier_semaphore()
    for peer in cols + rows_of:
        pl.semaphore_signal(barrier, inc=1, device_id=peer, device_id_type=MESH)
    moments = []
    for x in (xa, xb):
        v = x[...].astype(F32)
        moments += [jnp.sum(v, 1, keepdims=True), jnp.sum(v * v, 1, keepdims=True)]
    st_own[...] = lanes_of(moments)
    for i in range(columns // 128):
        gain_row[:, i * 128 : (i + 1) * 128] = gain[i : i + 1, :]
    sq[...] = jnp.zeros_like(sq)
    pl.semaphore_wait(barrier, len(cols) + len(rows_of))

    def block(j, owner):
        return full.at[j, pl.ds(owner * share, share), :]

    def spread(j, owner, slot, src, to_right, to_left):
        dst = block(j, owner)
        out = [(None, send(src, dst, s_sib.at[j, slot], recv.at[j, owner], sib))]
        if to_right:
            out.append((chip < chips - 1,
                        send(src, dst, s_right.at[j, slot], recv.at[j, owner], line(1))))
        if to_left:
            out.append((chip > 0,
                        send(src, dst, s_left.at[j, slot], recv.at[j, owner], line(-1))))
        return out

    def start(copies):
        for cond, copy in copies[::-1]:
            if cond is None:
                copy.start()
            else:
                pl.when(cond)(copy.start)

    def finish(copies):
        for cond, copy in copies:
            if cond is None:
                copy.wait_send()
            else:
                pl.when(cond)(copy.wait_send)

    mine_of = {2: spread(2, row, 0, go, True, True)}
    start(mine_of[2])
    st_copies = [send(st_own, st_in.at[i], st_s.at[i], st_r.at[i], p) for i, p in enumerate(cols)]
    for copy in st_copies:
        copy.start()
    block(2, row)[...] = go[...]

    def relays(j, visit, steps):
        for step in steps:
            for sign in (-1, 1):
                ok = chip >= step if sign < 0 else chip + step < chips

                @pl.when(ok)
                def _():
                    owner = row + 2 * sign * step
                    slot = step if sign < 0 else chips - 1 + step
                    visit(owner, sign, spread(j, owner, slot, block(j, owner), sign < 0, sign > 0))

    def gather(j, step):
        def visit(owner, sign, copies):
            arrived(block(j, owner), recv.at[j, owner], line(sign))
            start(copies)

        relays(j, visit, (step,))

    ends = (chip + 1) % chips < 2

    def gather_for(j, k):
        if k == 1:
            gather(j, 1)
        elif k == 2:
            pl.when(ends)(lambda: gather(j, 2))
        elif k == 3:
            pl.when(jnp.logical_not(ends))(lambda: gather(j, 2))
            pl.when(ends)(lambda: gather(j, 3))

    def hop(n, s):
        peer = peer_x if s in (0, 2, 3) else peer_y
        return (send(buf.at[n, s], inb.at[n, s], hop_s.at[n, s], hop_r.at[n, s], peer),
                send(buf_p.at[n, s], inb_p.at[n, s], peak_s.at[n, s], peak_r.at[n, s], peer))

    def go_hop(n, s, values):
        buf[n, s], buf_p[n, s] = encode(values)
        for copy in hop(n, s):
            copy.start()

    def got_hop(n, s):
        for copy in hop(n, s):
            copy.wait_recv()

    def over_tiles(body, size):
        @pl.loop(0, size // tile)
        def _(t):
            body(pl.ds(pl.multiple_of(t * tile, tile), tile))

    def item(j, k):
        return j * chips + k

    def place(j, k):
        return (3 * k + 2 - j) % 6

    def lanes(owner):
        return pl.ds(pl.multiple_of(owner * quarter, quarter), quarter)

    low_rows, high_rows = slice(0, upper), slice(upper, 2 * upper)

    def product(j, k):
        q = order(k)
        owner = 2 * q + 1 - core
        arrived(block(j, owner), recv.at[j, owner], sib)
        n, at_p = item(j, k), place(j, k)

        @pl.loop(0, 2)
        def _(h):
            at = pl.ds(pl.multiple_of(h * half, half), half)
            left = full[j, pl.ds(q * tokens, tokens), :]
            if j == 2:
                piece = lax.dot_general(left, w_down[at, :], (((1,), (1,)), ((), ())),
                                        preferred_element_type=F32)
            else:
                piece = jnp.dot(left, w_up[:, at], preferred_element_type=F32)
            partial[at_p, :, at] = piece

        go_hop(n, 0, partial[at_p, low_rows, lanes(diag)])
        go_hop(n, 1, partial[at_p, high_rows, lanes(diag)])
        go_hop(n, 2, partial[at_p, low_rows, lanes(flip_x)])
        go_hop(n, 5, partial[at_p, high_rows, lanes(flip_y)])

    def merge(j, k):
        n, at_p = item(j, k), place(j, k)
        got_hop(n, 0)
        go_hop(n, 4, partial[at_p, low_rows, lanes(flip_y)] + decode(inb[n, 0], inb_p[n, 0]))
        got_hop(n, 1)
        go_hop(n, 3, partial[at_p, high_rows, lanes(flip_x)] + decode(inb[n, 1], inb_p[n, 1]))

    def landed(j, k):
        for s in range(2, 6):
            got_hop(item(j, k), s)

    def summed(j, k, r, at, rows):
        n = item(j, k)
        first_s, second_s = ((2, 4), (5, 3))[r]
        return (partial[place(j, k), rows, lanes(col)]
                + decode(inb[n, first_s, at, :], inb_p[n, first_s])
                + decode(inb[n, second_s, at, :], inb_p[n, second_s]))

    chunk = 16

    def over(k, body):
        q = order(k)

        @pl.loop(0, upper // chunk)
        def _(i):
            at = pl.ds(pl.multiple_of(i * chunk, chunk), chunk)
            for r in range(2):
                rows = pl.ds(pl.multiple_of(r * upper + i * chunk, chunk), chunk)
                to = pl.ds(pl.multiple_of(q * tokens + r * upper + i * chunk, chunk), chunk)
                body(r, at, rows, to)

    def backward(k):
        landed(2, k)
        landed(1, k)

        def body(r, at, rows, to):
            v = summed(1, k, r, at, rows)
            phi = 0.5 * (1.0 + lax.erf(v * 0.7071067811865476))
            g = summed(2, k, r, at, rows)
            slope = phi + v * jnp.exp(-0.5 * v * v) * 0.3989422804014327
            acts[1, to, lanes(col)] = (v * phi).astype(BF16)
            acts[2, to, lanes(col)] = (g * slope).astype(BF16)

        over(k, body)
        publish(2, k)
        publish(1, k)

    def forward(k):
        landed(0, k)

        def body(r, at, rows, to):
            v = summed(0, k, r, at, rows)
            acts[0, to, lanes(col)] = (0.5 * v * (1.0 + lax.erf(v * 0.7071067811865476))).astype(BF16)

        over(k, body)
        publish(0, k)

    def piece_of(j, k, r, owner):
        rows = pl.ds(pl.multiple_of(order(k) * tokens + r * upper, upper), upper)
        return acts.at[j, rows, lanes(owner)]

    def passing(j, k, i):
        owner, r, peer = ((col, 0, peer_x), (col, 1, peer_y), (col, 1, peer_x), (col, 0, peer_y),
                          (flip_x, 0, peer_y), (flip_y, 1, peer_x))[i]
        ref, n = piece_of(j, k, r, owner), item(j, k)
        return send(ref, ref, g_s.at[n, i], g_r.at[n, i], peer)

    def publish(j, k):
        for i in range(4):
            passing(j, k, i).start()

    def got_piece(j, k, i):
        owner, r = ((flip_x, 0), (flip_y, 1), (flip_x, 1), (flip_y, 0), (diag, 0), (diag, 1))[i]
        arrived(piece_of(j, k, r, owner), g_r.at[item(j, k), i], peer_x)

    def pass_on(j, k):
        got_piece(j, k, 0)
        passing(j, k, 4).start()
        got_piece(j, k, 1)
        passing(j, k, 5).start()

    def complete(j, k):
        for i in range(2, 6):
            got_piece(j, k, i)

    def to_sib(j, k):
        return send(part.at[j, k, 1 - core], from_sib.at[j, k], sib_s.at[j, k], sib_r.at[j, k], sib)

    def to_owner(j, k, h):
        peer, slot = {"row": 2 * order(k) + core, "col": col}, min(k, 2) - 1
        return (send(zbuf.at[j, k, h], zin.at[j, slot, h], z_s.at[j, k, h], z_r.at[j, slot, h], peer),
                send(zbuf_p.at[j, k, h], zin_p.at[j, slot, h], zp_s.at[j, k, h], zp_r.at[j, slot, h], peer))

    def to_middle(j, k, h):
        peer = {"row": row + 2 - 4 * high, "col": col}
        return (send(zbuf.at[j, k, h], zmid.at[j, k - 2, h], z_s.at[j, k, h], zm_r.at[j, k - 2, h], peer),
                send(zbuf_p.at[j, k, h], zmid_p.at[j, k - 2, h], zp_s.at[j, k, h], zmp_r.at[j, k - 2, h], peer))

    def second(j, k):
        @pl.loop(0, 2)
        def _(h):
            at = pl.ds(pl.multiple_of(h * half, half), half)
            left = acts[2 * j, pl.ds(pl.multiple_of(order(k) * tokens, tokens), tokens), :]
            if j == 0:
                piece = jnp.dot(left, w_down[:, at], preferred_element_type=F32)
            else:
                piece = lax.dot_general(left, w_up[at, :], (((1,), (1,)), ((), ())),
                                        preferred_element_type=F32)
            part[j, k, 0, :, at] = piece[:share]
            part[j, k, 1, :, at] = piece[share:]

        to_sib(j, k).start()

    def in_half(h, at):
        return pl.ds(pl.multiple_of(h * half + at * tile, tile), tile)

    def code(j, k, h, more, copies):
        @pl.loop(0, half // tile)
        def _(t):
            at, wide_at = pl.ds(pl.multiple_of(t * tile, tile), tile), in_half(h, t)
            values = part[j, k, core, :, wide_at] + from_sib[j, k, :, wide_at]
            if more:
                values = values + decode(zmid[j, k - 2, h, :, at], zmid_p[j, k - 2, h, :, at])
            zbuf[j, k, h, :, at], zbuf_p[j, k, h, :, at] = encode(values)

        for copy in copies:
            copy.start()

    def onward(j, k):
        to_sib(j, k).wait_recv()
        if k == 0:
            mine[j] = part[j, k, core] + from_sib[j, k]
        elif k == 1:
            for h in range(2):
                code(j, k, h, False, to_owner(j, k, h))
        else:
            @pl.when(ends)
            def _():
                for h in range(2):
                    code(j, k, h, False, to_middle(j, k, h))

    def join(j, k):
        @pl.when(jnp.logical_not(ends))
        def _():
            for h in range(2):
                for copy in to_middle(j, k, h):
                    copy.wait_recv()
                code(j, k, h, True, to_owner(j, k, h))

    def collect(j):
        for slot in range(2):
            for h in range(2):
                for copy in to_owner(j, slot + 1, h):
                    copy.wait_recv()
                across = slice(h * half, (h + 1) * half)
                mine[j, :, across] = mine[j, :, across] + decode(zin[j, slot, h], zin_p[j, slot, h])

    def gradient(out, left, right):
        step_m, step_n = 256, half

        @pl.loop(0, out.shape[0] // step_m)
        def _(m):
            at = pl.ds(pl.multiple_of(m * step_m, step_m), step_m)
            for n in range(out.shape[1] // step_n):
                across = slice(n * step_n, (n + 1) * step_n)
                piece = lax.dot_general(left[:, at], right[:, across], (((0,), (0,)), ((), ())),
                                        preferred_element_type=F32)
                out[at, across] = piece
                sq[:, across] = sq[:, across] + jnp.sum(piece * piece, 0, keepdims=True)

    load_down.wait()
    product(2, 0)
    for copy in st_copies:
        copy.wait()
    stats = st_own[...]
    for i in range(C - 1):
        stats = stats + st_in[i]
    for j, x, at in ((1, xb, 2), (0, xa, 0)):
        hat, _ = normal_of(x[...].astype(F32), stats, at, width)
        block(j, row)[...] = (hat * gain_row[...]).astype(BF16)
        mine_of[j] = spread(j, row, 0, block(j, row), True, True)
        start(mine_of[j])
    load_up.wait()
    product(1, 0)
    merge(2, 0)
    product(0, 0)
    merge(1, 0)
    gather_for(2, 1)
    product(2, 1)
    merge(0, 0)
    backward(0)
    gather_for(1, 1)
    product(1, 1)
    merge(2, 1)
    forward(0)
    gather_for(0, 1)
    product(0, 1)
    merge(1, 1)
    pass_on(2, 0)
    pass_on(1, 0)
    gather_for(2, 2)
    product(2, 2)
    merge(0, 1)
    backward(1)
    pass_on(0, 0)
    gather_for(1, 2)
    product(1, 2)
    merge(2, 2)
    forward(1)
    complete(2, 0)
    second(1, 0)
    gather_for(0, 2)
    product(0, 2)
    merge(1, 2)
    pass_on(2, 1)
    pass_on(1, 1)
    complete(0, 0)
    second(0, 0)
    onward(1, 0)
    gather_for(2, 3)
    product(2, 3)
    merge(0, 2)
    backward(2)
    pass_on(0, 1)
    gather_for(1, 3)
    product(1, 3)
    merge(2, 3)
    forward(2)
    complete(2, 1)
    second(1, 1)
    gather_for(0, 3)
    product(0, 3)
    merge(1, 3)
    onward(0, 0)
    pass_on(2, 2)
    pass_on(1, 2)
    complete(0, 1)
    second(0, 1)
    onward(1, 1)
    merge(0, 3)
    backward(3)
    pass_on(0, 2)
    forward(3)
    complete(2, 2)
    second(1, 2)
    onward(0, 1)
    pass_on(2, 3)
    pass_on(1, 3)
    onward(1, 2)
    complete(0, 2)
    second(0, 2)
    pass_on(0, 3)
    onward(0, 2)
    complete(2, 3)
    second(1, 3)
    join(1, 2)
    onward(1, 3)
    complete(0, 3)
    second(0, 3)
    join(0, 2)
    onward(0, 3)
    gradient(g_up, full.at[1], acts.at[2])
    join(1, 3)
    for k in range(chips):
        complete(1, k)
    gradient(g_down, acts.at[1], full.at[2])
    join(0, 3)
    tt_own[...] = jnp.broadcast_to(jnp.sum(sq[...], 1, keepdims=True), tt_own.shape)
    third = [send(tt_own, tt_in.at[row], tt_s.at[i], tt_r.at[i], p) for i, p in enumerate(rows_of)]
    for copy in third:
        copy.start()
    collect(1)
    grad = mine[1]
    hat, inv = normal_of(xb[...].astype(F32), stats, 2, width)
    scaled = grad * gain_row[...]
    back_own[...] = lanes_of([jnp.sum(scaled, 1, keepdims=True), jnp.sum(scaled * hat, 1, keepdims=True)])
    first = [send(back_own, back_in.at[i], back_s.at[i], back_r.at[i], p) for i, p in enumerate(cols)]
    for copy in first:
        copy.start()
    gain_part = jnp.sum(grad * hat, 0, keepdims=True)
    for i in range(columns // 128):
        gp_own[i : i + 1, :] = gain_part[:, i * 128 : (i + 1) * 128]
    gains_out = [send(gp_own, gp_in.at[row], gp_s.at[i], gp_r.at[i], p) for i, p in enumerate(rows_of)]
    for copy in gains_out:
        copy.start()
    gp_in[row] = gp_own[...]
    tt_in[row] = tt_own[...]
    for copy in gains_out + third:
        copy.wait()
    gains, squares = gp_in[0], tt_in[0]
    for i in range(1, R):
        gains, squares = gains + gp_in[i], squares + tt_in[i]
    gained[...] = gains
    uu_own[...] = squares + jnp.sum(gains * gains)
    fourth = [send(uu_own, uu_in.at[col], uu_s.at[i], uu_r.at[i], p) for i, p in enumerate(cols)]
    for copy in fourth:
        copy.start()
    uu_in[col] = uu_own[...]
    for copy in first:
        copy.wait()
    sums = back_own[...]
    for i in range(C - 1):
        sums = sums + back_in[i]
    c1, c2 = sums[:, 0:1] / width, sums[:, 1:2] / width
    hat, inv = normal_of(xb[...].astype(F32), stats, 2, width)
    scaled = mine[1] * gain_row[...]
    dx[...] = (go[...].astype(F32) + inv * (scaled - c1 - hat * c2)).astype(BF16)
    for copy in fourth:
        copy.wait()
    total = uu_in[0]
    for i in range(1, C):
        total = total + uu_in[i]
    norm_value = jnp.sqrt(total)
    verdict[0] = jnp.minimum(1.0, clip_share * math.sqrt(params) / norm_value)
    verdict[1] = norm_value / math.sqrt(params)
    collect(0)
    y[...] = (xa[...].astype(F32) + mine[0]).astype(BF16)

    for j in (2, 1, 0):
        finish(mine_of[j])
        relays(j, lambda owner, sign, copies: finish(copies), range(1, chips))
        for k in range(chips):
            for i in range(6):
                passing(j, k, i).wait_send()
                for copy in hop(item(j, k), i):
                    copy.wait_send()
    for j in (0, 1):
        for i in range(chips):
            to_sib(j, i).wait_send()
            for h in range(2):
                if i == 1:
                    for copy in to_owner(j, i, h):
                        copy.wait_send()
                elif i > 1:
                    for copy in to_middle(j, i, h):
                        copy.wait_send()


def step_on_core(R, C, width, params, x_fwd, x_bwd, grad_out, gain, w_up, w_down):
    rows, columns = x_fwd.shape
    wide = w_up.shape[1]
    chips, slots = R // 2, 2 * (R // 2) - 1
    count = rows * R
    tokens, half = count // C, wide // 2
    lines = columns // 128
    VM = pltpu.VMEM
    return pl.pallas_call(
        functools.partial(step_kernel, R, C, width, params),
        out_shape=(VM((columns, wide), F32), VM((wide, columns), F32), VM((rows, columns), BF16),
                   VM((rows, columns), BF16), VM((lines, 128), F32), VM((2, 8, 128), F32)),
        in_specs=[VMEM] * 4 + [pl.BlockSpec(memory_space=pl.ANY)] * 2,
        out_specs=(VMEM,) * 6,
        scratch_shapes=[
            VM((3, count, columns), BF16), VM((3, count, wide), BF16),
            VM(w_up.shape, BF16), VM(w_down.shape, BF16), VM((1, columns), F32),
            VM((rows, 128), F32), VM((C - 1, rows, 128), F32),
            VM((6, tokens, wide), F32),
            VM((12, 6, tokens // 2, wide // C), BF16), VM((12, 6, tokens // 2, wide // C), BF16),
            VM((12, 6, 1, wide // C), F32), VM((12, 6, 1, wide // C), F32),
            VM((2, chips, 2, rows, columns), F32), VM((2, chips, rows, columns), F32),
            VM((2, chips, 2, rows, half), BF16), VM((2, 2, 2, rows, half), BF16),
            VM((2, 2, 2, rows, half), BF16), VM((2, chips, 2, 1, half), F32),
            VM((2, 2, 2, 1, half), F32), VM((2, 2, 2, 1, half), F32),
            VM((2, rows, columns), F32), VM((1, columns), F32),
            VM((rows, 128), F32), VM((C - 1, rows, 128), F32),
            VM((lines, 128), F32), VM((R, lines, 128), F32),
            VM((8, 128), F32), VM((R, 8, 128), F32), VM((8, 128), F32), VM((C, 8, 128), F32),
        ]
        + [DMA((2,)), DMA((C - 1,)), DMA((C - 1,)),
           DMA((3, slots)), DMA((3, slots)), DMA((3, slots)), DMA((3, R))]
        + [DMA((12, 6))] * 6 + [DMA((2, chips))] * 2
        + [DMA((2, chips, 2)), DMA((2, 2, 2))] * 2 + [DMA((2, 2, 2))] * 2
        + [DMA((C - 1,))] * 2 + [DMA((R - 1,))] * 4 + [DMA((C - 1,))] * 2,
        compiler_params=pltpu.CompilerParams(
            collective_id=0, has_side_effects=True, vmem_limit_bytes=GRANT),
        cost_estimate=pl.CostEstimate(flops=2 * 10**10, bytes_accessed=10**7, transcendentals=0),
    )(x_fwd, x_bwd, grad_out, gain, w_up, w_down)


def clip_kernel(g_up, g_down, y_in, dx_in, gains, verdict, up, down, y, dx, step_gain, rms, staged, sem):
    factor = verdict[0, 0:1, 0:1]
    slots = staged.shape[1]
    size = staged.shape[2]
    for which, (grad, out) in enumerate(((g_up, up), (g_down, down))):
        for i in range(slots):
            at = pl.ds(i * size, size)
            staged[which, i] = grad[at, :] * factor
            pltpu.make_async_copy(staged.at[which, i], out.at[at, :], sem.at[which, i]).start()
    y[...] = y_in[...]
    dx[...] = dx_in[...]
    step_gain[...] = gains[...] * factor
    rms[...] = verdict[1, 0:1, 0:1]
    for which, out in enumerate((up, down)):
        for i in range(slots):
            at = pl.ds(i * size, size)
            pltpu.make_async_copy(staged.at[which, i], out.at[at, :], sem.at[which, i]).wait()


def clip(g_up, g_down, y, dx, gains, verdict):
    slots = 12
    size = g_up.shape[0] // slots
    like = jax.ShapeDtypeStruct
    return pl.pallas_call(
        clip_kernel,
        out_shape=(like(g_up.shape, F32), like(g_down.shape, F32), like(y.shape, BF16),
                   like(dx.shape, BF16), like(gains.shape, F32), like((1, 1), F32)),
        in_specs=[VMEM] * 6,
        out_specs=(pl.BlockSpec(memory_space=pl.ANY),) * 2 + (VMEM,) * 4,
        scratch_shapes=[pltpu.VMEM((2, slots, size, g_up.shape[1]), F32), DMA((2, slots))],
        compiler_params=pltpu.CompilerParams(vmem_limit_bytes=20 * 1024 * 1024),
        cost_estimate=pl.CostEstimate(flops=10**8, bytes_accessed=4 * 10**7, transcendentals=0),
    )(*(pltpu.with_memory_space_constraint(v, pltpu.VMEM) for v in (g_up, g_down, y, dx, gains, verdict)))


def with_kernels(R, C):
    def step(x_fwd, x_bwd, grad_out, gain, w_up, w_down):
        rows, columns = x_fwd.shape
        width = columns * C
        params = 2 * width * w_up.shape[1] * R + width
        parts = step_on_core(R, C, width, params, x_fwd, x_bwd, grad_out,
                             gain.reshape(columns // 128, 128), w_up, w_down)
        up, down, y, dx, step_gain, rms = clip(*parts)
        return y, dx, up, down, step_gain.reshape(columns), rms.reshape(())

    return step


def solution(mesh):
    placed = (
        P("row", "col"),
        P("row", "col"),
        P("row", "col"),
        P("col"),
        P("col", "row"),
        P("row", "col"),
    )
    R, C = mesh.shape["row"], mesh.shape["col"]
    body = with_kernels(R, C) if C == 4 and R == 8 else on_device
    return jax.shard_map(
        body,
        mesh=mesh,
        in_specs=placed,
        out_specs=(
            P("row", "col"),
            P("row", "col"),
            P("col", "row"),
            P("row", "col"),
            P("col"),
            P(),
        ),
        check_vma=False,
    )
```

```python
import functools
import math

import jax
import jax.numpy as jnp
from jax import lax
from jax.experimental import pallas as pl
from jax.experimental.pallas import tpu as pltpu
from jax.sharding import PartitionSpec as P

D = 6144
FF = 12288


eps = 1e-06
clip_share = 0.25


def erf_gelu(value):
    return 0.5 * value * (1.0 + lax.erf(value * 0.7071067811865476))


def gelu_slope(value):
    return (
        0.5 * (1.0 + lax.erf(value * 0.7071067811865476))
        + value * jnp.exp(-0.5 * value * value) * 0.3989422804014327
    )


def contract(left, right, left_dim, right_dim):
    return lax.dot_general(
        left, right, (((left_dim,), (right_dim,)), ((), ())), preferred_element_type=jnp.float32
    )


def row_sums(tokens):
    values = tokens.astype(jnp.float32)
    return (jnp.sum(values, -1), jnp.sum(values * values, -1))


def normalize(tokens, first, second):
    values = tokens.astype(jnp.float32)
    centre = first / D
    spread = second / D - centre * centre
    inv_scale = lax.rsqrt(spread + eps)
    return ((values - centre[:, None]) * inv_scale[:, None], inv_scale)


def up_both(normed_a, normed_b, w_up):
    full_a, full_b = (
        lax.all_gather(normed_a, "row", axis=0, tiled=True),
        lax.all_gather(normed_b, "row", axis=0, tiled=True),
    )
    width = w_up.shape[1]
    summed = lax.psum_scatter(
        jnp.concatenate(
            [
                jnp.dot(full_a, w_up, preferred_element_type=jnp.float32),
                jnp.dot(full_b, w_up, preferred_element_type=jnp.float32),
            ],
            1,
        ),
        "col",
        scatter_dimension=0,
        tiled=True,
    )
    return (summed[:, :width], summed[:, width:], full_b)


def on_device(x_fwd, x_bwd, grad_out, gain, w_up, w_down):
    first_a, second_a = row_sums(x_fwd)
    first_b, second_b = row_sums(x_bwd)
    first_a, second_a, first_b, second_b = lax.psum((first_a, second_a, first_b, second_b), "col")
    centred_a, _ = normalize(x_fwd, first_a, second_a)
    centred_b, inv_scale = normalize(x_bwd, first_b, second_b)
    normed_a = (centred_a * gain).astype(jnp.bfloat16)
    normed_b = (centred_b * gain).astype(jnp.bfloat16)
    pre_a, pre_b, normed_full = up_both(normed_a, normed_b, w_up)
    hidden_a = erf_gelu(pre_a).astype(jnp.bfloat16)
    output_part = jnp.dot(
        lax.all_gather(hidden_a, "col", axis=0, tiled=True),
        w_down,
        preferred_element_type=jnp.float32,
    )
    output_sum = lax.psum_scatter(output_part, "row", scatter_dimension=0, tiled=True)
    y_fwd = (x_fwd.astype(jnp.float32) + output_sum).astype(jnp.bfloat16)
    hidden_b = erf_gelu(pre_b).astype(jnp.bfloat16)
    grad_full = lax.all_gather(grad_out, "row", axis=0, tiled=True)
    grad_hidden = lax.psum_scatter(
        contract(grad_full, w_down, 1, 1), "col", scatter_dimension=0, tiled=True
    )
    grad_pre = (grad_hidden * gelu_slope(pre_b)).astype(jnp.bfloat16)
    hidden_piece = lax.all_gather(hidden_b, "col", axis=0, tiled=True)
    pre_piece = lax.all_gather(grad_pre, "col", axis=0, tiled=True)
    down_total = contract(hidden_piece, grad_full, 0, 0)
    up_total = contract(normed_full, pre_piece, 0, 0)
    input_total = contract(pre_piece, w_up, 1, 1)
    grad_normed = lax.psum_scatter(input_total, "row", scatter_dimension=0, tiled=True)
    scaled = grad_normed * gain
    first_back = jnp.sum(scaled, -1)
    second_back = jnp.sum(scaled * centred_b, -1)
    first_back, second_back = lax.psum((first_back, second_back), "col")
    dx_bwd = (
        grad_out.astype(jnp.float32)
        + inv_scale[:, None]
        * (scaled - first_back[:, None] / D - centred_b * (second_back[:, None] / D))
    ).astype(jnp.bfloat16)
    gain_part = jnp.sum(grad_normed * centred_b, 0)
    weight_squares = jnp.sum(up_total * up_total) + jnp.sum(down_total * down_total)
    g_gain = lax.psum(gain_part, "row")
    first_row = (lax.axis_index("row") == 0).astype(jnp.float32)
    total = lax.psum(weight_squares + first_row * jnp.sum(g_gain * g_gain), ("row", "col"))
    param_count = 2 * D * FF + D
    norm_value = jnp.sqrt(total)
    grad_rms = norm_value / math.sqrt(param_count)
    factor = jnp.minimum(1.0, clip_share * math.sqrt(param_count) / norm_value)
    return (y_fwd, dx_bwd, up_total * factor, down_total * factor, g_gain * factor, grad_rms)


MESH = pl.DeviceIdType.MESH
VMEM = pl.BlockSpec(memory_space=pltpu.VMEM)
F32 = jnp.float32
BF16 = jnp.bfloat16
DMA = pltpu.SemaphoreType.DMA
GRANT = 45 * 1024 * 1024


def send(src, dst, send_sem, recv_sem, peer):
    return pltpu.make_async_remote_copy(
        src_ref=src, dst_ref=dst, send_sem=send_sem, recv_sem=recv_sem,
        device_id=peer, device_id_type=MESH,
    )


def arrived(ref, sem, peer):
    pltpu.make_async_remote_copy(
        src_ref=ref, dst_ref=ref, send_sem=sem, recv_sem=sem,
        device_id=peer, device_id_type=MESH,
    ).wait_recv()


SPAN = 252.0


def encode(values):
    size = jnp.abs(values)
    peak = jnp.maximum(jnp.max(size, 0, keepdims=True), 1e-30)
    code = jnp.exp2(size * (SPAN / peak) - 0.5 * SPAN)
    return jnp.where(values < 0.0, -code, code).astype(BF16), peak


def decode(codes, peak):
    code = codes.astype(F32)
    size = jnp.log(jnp.abs(code)) * (peak * (1.4426950408889634 / SPAN)) + 0.5 * peak
    return jnp.where(code < 0.0, -size, size)


def normal_of(values, stats, at, width):
    centre = stats[:, at : at + 1] / width
    spread = stats[:, at + 1 : at + 2] / width - centre * centre
    inv = lax.rsqrt(spread + eps)
    return (values - centre) * inv, inv


def lanes_of(columns):
    rows = columns[0].shape[0]
    lane = lax.broadcasted_iota(jnp.int32, (rows, 128), 1)
    out = jnp.zeros((rows, 128), F32)
    for i, column in enumerate(columns):
        out = jnp.where(lane == i, column, out)
    return out


def step_kernel(R, C, width, params, xa, xb, go, gain, w_up_hbm, w_down_hbm,
                g_up, g_down, y, dx, gained, verdict,
                full, acts, w_up, w_down, gain_row, st_own, st_in, partial, buf, inb, buf_p, inb_p,
                part, from_sib, zbuf, zin, zmid, zbuf_p, zin_p, zmid_p, mine, sq,
                back_own, back_in, gp_own, gp_in, uu_own, uu_in,
                w_sem, st_s, st_r, s_right, s_left, s_sib, recv, hop_s, hop_r, peak_s, peak_r,
                g_s, g_r, sib_s, sib_r, z_s, z_r, zp_s, zp_r, zm_r, zmp_r,
                back_s, back_r, gp_s, gp_r, uu_s, uu_r):
    row, col = lax.axis_index("row"), lax.axis_index("col")
    chips = R // 2
    chip, core = row // 2, row % 2
    sib = {"row": row + 1 - 2 * core, "col": col}
    cols = [{"row": row, "col": (col + i) % C} for i in range(1, C)]
    rows_of = [{"row": (row + i) % R, "col": col} for i in range(1, R)]
    flip_x = col + 1 - 2 * (col % 2)
    flip_y = (col + 2) % 4
    diag = 3 - col
    peer_x, peer_y = {"row": row, "col": flip_x}, {"row": row, "col": flip_y}
    share, columns = xa.shape
    tokens = share * R // C
    wide = w_up.shape[1]
    half = wide // 2
    quarter = wide // C
    upper = tokens // 2
    tile = half // 2
    high = chip // 2

    def line(step):
        return {"row": row + 2 * step, "col": col}

    def mirror(at, on):
        return at + on * (chips - 1 - 2 * at)

    def order(k):
        low = mirror(chip, high)
        return mirror((low, 1 - low, 2, 3)[k], high)

    load_up = pltpu.make_async_copy(w_up_hbm, w_up, w_sem.at[0])
    load_down = pltpu.make_async_copy(w_down_hbm, w_down, w_sem.at[1])
    load_down.start()
    load_up.start()
    barrier = pltpu.get_barrier_semaphore()
    for peer in cols + rows_of:
        pl.semaphore_signal(barrier, inc=1, device_id=peer, device_id_type=MESH)
    moments = []
    for x in (xa, xb):
        v = x[...].astype(F32)
        moments += [jnp.sum(v, 1, keepdims=True), jnp.sum(v * v, 1, keepdims=True)]
    st_own[...] = lanes_of(moments)
    for i in range(columns // 128):
        gain_row[:, i * 128 : (i + 1) * 128] = gain[i : i + 1, :]
    sq[...] = jnp.zeros_like(sq)
    pl.semaphore_wait(barrier, len(cols) + len(rows_of))

    def block(j, owner):
        return full.at[j, pl.ds(owner * share, share), :]

    def spread(j, owner, slot, src, to_right, to_left):
        dst = block(j, owner)
        out = [(None, send(src, dst, s_sib.at[j, slot], recv.at[j, owner], sib))]
        if to_right:
            out.append((chip < chips - 1,
                        send(src, dst, s_right.at[j, slot], recv.at[j, owner], line(1))))
        if to_left:
            out.append((chip > 0,
                        send(src, dst, s_left.at[j, slot], recv.at[j, owner], line(-1))))
        return out

    def start(copies):
        for cond, copy in copies[::-1]:
            if cond is None:
                copy.start()
            else:
                pl.when(cond)(copy.start)

    def finish(copies):
        for cond, copy in copies:
            if cond is None:
                copy.wait_send()
            else:
                pl.when(cond)(copy.wait_send)

    mine_of = {2: spread(2, row, 0, go, True, True)}
    start(mine_of[2])
    st_copies = [send(st_own, st_in.at[i], st_s.at[i], st_r.at[i], p) for i, p in enumerate(cols)]
    for copy in st_copies:
        copy.start()
    block(2, row)[...] = go[...]

    def relays(j, visit, steps):
        for step in steps:
            for sign in (-1, 1):
                ok = chip >= step if sign < 0 else chip + step < chips

                @pl.when(ok)
                def _():
                    owner = row + 2 * sign * step
                    slot = step if sign < 0 else chips - 1 + step
                    visit(owner, sign, spread(j, owner, slot, block(j, owner), sign < 0, sign > 0))

    def gather(j, step):
        def visit(owner, sign, copies):
            arrived(block(j, owner), recv.at[j, owner], line(sign))
            start(copies)

        relays(j, visit, (step,))

    ends = (chip + 1) % chips < 2

    def gather_for(j, k):
        if k < 3:
            gather(j, k)
        else:
            pl.when(ends)(lambda: gather(j, 3))

    def hop(n, s):
        peer = peer_x if s in (0, 2, 3) else peer_y
        return (send(buf.at[n, s], inb.at[n, s], hop_s.at[n, s], hop_r.at[n, s], peer),
                send(buf_p.at[n, s], inb_p.at[n, s], peak_s.at[n, s], peak_r.at[n, s], peer))

    def go_hop(n, s, values):
        buf[n, s], buf_p[n, s] = encode(values)
        for copy in hop(n, s):
            copy.start()

    def got_hop(n, s):
        for copy in hop(n, s):
            copy.wait_recv()

    def over_tiles(body, size):
        @pl.loop(0, size // tile)
        def _(t):
            body(pl.ds(pl.multiple_of(t * tile, tile), tile))

    def item(j, k):
        return j * chips + k

    def place(j, k):
        return 4 + k % 2 if j == 0 else (2 * k + 2 - j) % 4

    def lanes(owner):
        return pl.ds(pl.multiple_of(owner * quarter, quarter), quarter)

    low_rows, high_rows = slice(0, upper), slice(upper, 2 * upper)

    def product(j, k):
        q = order(k)
        owner = 2 * q + 1 - core
        arrived(block(j, owner), recv.at[j, owner], sib)
        n, at_p = item(j, k), place(j, k)

        @pl.loop(0, 2)
        def _(h):
            at = pl.ds(pl.multiple_of(h * half, half), half)
            left = full[j, pl.ds(q * tokens, tokens), :]
            if j == 2:
                piece = lax.dot_general(left, w_down[at, :], (((1,), (1,)), ((), ())),
                                        preferred_element_type=F32)
            else:
                piece = jnp.dot(left, w_up[:, at], preferred_element_type=F32)
            partial[at_p, :, at] = piece

        go_hop(n, 0, partial[at_p, low_rows, lanes(diag)])
        go_hop(n, 1, partial[at_p, high_rows, lanes(diag)])
        go_hop(n, 2, partial[at_p, low_rows, lanes(flip_x)])
        go_hop(n, 5, partial[at_p, high_rows, lanes(flip_y)])

    def merge(j, k):
        n, at_p = item(j, k), place(j, k)
        got_hop(n, 0)
        go_hop(n, 4, partial[at_p, low_rows, lanes(flip_y)] + decode(inb[n, 0], inb_p[n, 0]))
        got_hop(n, 1)
        go_hop(n, 3, partial[at_p, high_rows, lanes(flip_x)] + decode(inb[n, 1], inb_p[n, 1]))

    def landed(j, k):
        for s in range(2, 6):
            got_hop(item(j, k), s)

    def summed(j, k, r, at, rows):
        n = item(j, k)
        first_s, second_s = ((2, 4), (5, 3))[r]
        return (partial[place(j, k), rows, lanes(col)]
                + decode(inb[n, first_s, at, :], inb_p[n, first_s])
                + decode(inb[n, second_s, at, :], inb_p[n, second_s]))

    chunk = 16

    def over(k, body):
        q = order(k)

        @pl.loop(0, upper // chunk)
        def _(i):
            at = pl.ds(pl.multiple_of(i * chunk, chunk), chunk)
            for r in range(2):
                rows = pl.ds(pl.multiple_of(r * upper + i * chunk, chunk), chunk)
                to = pl.ds(pl.multiple_of(q * tokens + r * upper + i * chunk, chunk), chunk)
                body(r, at, rows, to)

    def backward(k):
        landed(2, k)
        landed(1, k)

        def body(r, at, rows, to):
            v = summed(1, k, r, at, rows)
            phi = 0.5 * (1.0 + lax.erf(v * 0.7071067811865476))
            g = summed(2, k, r, at, rows)
            slope = phi + v * jnp.exp(-0.5 * v * v) * 0.3989422804014327
            acts[1, to, lanes(col)] = (v * phi).astype(BF16)
            acts[2, to, lanes(col)] = (g * slope).astype(BF16)

        over(k, body)
        publish(2, k)
        publish(1, k)

    def forward(k):
        landed(0, k)

        def body(r, at, rows, to):
            v = summed(0, k, r, at, rows)
            acts[0, to, lanes(col)] = (0.5 * v * (1.0 + lax.erf(v * 0.7071067811865476))).astype(BF16)

        over(k, body)
        publish(0, k)

    def piece_of(j, k, r, owner):
        rows = pl.ds(pl.multiple_of(order(k) * tokens + r * upper, upper), upper)
        return acts.at[j, rows, lanes(owner)]

    def passing(j, k, i):
        owner, r, peer = ((col, 0, peer_x), (col, 1, peer_y), (col, 1, peer_x), (col, 0, peer_y),
                          (flip_x, 0, peer_y), (flip_y, 1, peer_x))[i]
        ref, n = piece_of(j, k, r, owner), item(j, k)
        return send(ref, ref, g_s.at[n, i], g_r.at[n, i], peer)

    def publish(j, k):
        for i in range(4):
            passing(j, k, i).start()

    def got_piece(j, k, i):
        owner, r = ((flip_x, 0), (flip_y, 1), (flip_x, 1), (flip_y, 0), (diag, 0), (diag, 1))[i]
        arrived(piece_of(j, k, r, owner), g_r.at[item(j, k), i], peer_x)

    def pass_on(j, k):
        got_piece(j, k, 0)
        passing(j, k, 4).start()
        got_piece(j, k, 1)
        passing(j, k, 5).start()

    def complete(j, k):
        for i in range(2, 6):
            got_piece(j, k, i)

    def to_sib(j, k):
        return send(part.at[j, k, 1 - core], from_sib.at[j, k], sib_s.at[j, k], sib_r.at[j, k], sib)

    def to_owner(j, k, h):
        peer, slot = {"row": 2 * order(k) + core, "col": col}, min(k, 2) - 1
        return (send(zbuf.at[j, k, h], zin.at[j, slot, h], z_s.at[j, k, h], z_r.at[j, slot, h], peer),
                send(zbuf_p.at[j, k, h], zin_p.at[j, slot, h], zp_s.at[j, k, h], zp_r.at[j, slot, h], peer))

    def to_middle(j, k, h):
        peer = {"row": row + 2 - 4 * high, "col": col}
        return (send(zbuf.at[j, k, h], zmid.at[j, k - 2, h], z_s.at[j, k, h], zm_r.at[j, k - 2, h], peer),
                send(zbuf_p.at[j, k, h], zmid_p.at[j, k - 2, h], zp_s.at[j, k, h], zmp_r.at[j, k - 2, h], peer))

    def second(j, k):
        @pl.loop(0, 2)
        def _(h):
            at = pl.ds(pl.multiple_of(h * half, half), half)
            left = acts[2 * j, pl.ds(pl.multiple_of(order(k) * tokens, tokens), tokens), :]
            if j == 0:
                piece = jnp.dot(left, w_down[:, at], preferred_element_type=F32)
            else:
                piece = lax.dot_general(left, w_up[at, :], (((1,), (1,)), ((), ())),
                                        preferred_element_type=F32)
            part[j, k, 0, :, at] = piece[:share]
            part[j, k, 1, :, at] = piece[share:]

        to_sib(j, k).start()

    def in_half(h, at):
        return pl.ds(pl.multiple_of(h * half + at * tile, tile), tile)

    def code(j, k, h, more, copies):
        @pl.loop(0, half // tile)
        def _(t):
            at, wide_at = pl.ds(pl.multiple_of(t * tile, tile), tile), in_half(h, t)
            values = part[j, k, core, :, wide_at] + from_sib[j, k, :, wide_at]
            if more:
                values = values + decode(zmid[j, k - 2, h, :, at], zmid_p[j, k - 2, h, :, at])
            zbuf[j, k, h, :, at], zbuf_p[j, k, h, :, at] = encode(values)

        for copy in copies:
            copy.start()

    def onward(j, k):
        to_sib(j, k).wait_recv()
        if k == 0:
            mine[j] = part[j, k, core] + from_sib[j, k]
        elif k == 1:
            for h in range(2):
                code(j, k, h, False, to_owner(j, k, h))
        else:
            @pl.when(ends)
            def _():
                for h in range(2):
                    code(j, k, h, False, to_middle(j, k, h))

    def join(j, k):
        @pl.when(jnp.logical_not(ends))
        def _():
            for h in range(2):
                for copy in to_middle(j, k, h):
                    copy.wait_recv()
                code(j, k, h, True, to_owner(j, k, h))

    def collect(j):
        for slot in range(2):
            for h in range(2):
                for copy in to_owner(j, slot + 1, h):
                    copy.wait_recv()
                across = slice(h * half, (h + 1) * half)
                mine[j, :, across] = mine[j, :, across] + decode(zin[j, slot, h], zin_p[j, slot, h])

    def gradient(out, left, right, part_of):
        step_m, step_n = 256, half
        blocks = out.shape[0] // step_m // 2

        @pl.loop(part_of * blocks, (part_of + 1) * blocks)
        def _(m):
            at = pl.ds(pl.multiple_of(m * step_m, step_m), step_m)
            for n in range(out.shape[1] // step_n):
                across = slice(n * step_n, (n + 1) * step_n)
                piece = lax.dot_general(left[:, at], right[:, across], (((0,), (0,)), ((), ())),
                                        preferred_element_type=F32)
                out[at, across] = piece
                sq[:, across] = sq[:, across] + jnp.sum(piece * piece, 0, keepdims=True)

    load_down.wait()
    product(2, 0)
    for copy in st_copies:
        copy.wait()
    stats = st_own[...]
    for i in range(C - 1):
        stats = stats + st_in[i]
    for j, x, at in ((1, xb, 2), (0, xa, 0)):
        hat, _ = normal_of(x[...].astype(F32), stats, at, width)
        block(j, row)[...] = (hat * gain_row[...]).astype(BF16)
        mine_of[j] = spread(j, row, 0, block(j, row), True, True)
        start(mine_of[j])
    load_up.wait()
    product(1, 0)
    merge(2, 0)
    product(0, 0)
    merge(1, 0)
    gather_for(2, 1)
    product(2, 1)
    backward(0)
    gather_for(1, 1)
    product(1, 1)
    merge(2, 1)
    gather_for(0, 1)
    merge(0, 0)
    pass_on(2, 0)
    pass_on(1, 0)
    merge(1, 1)
    gather_for(2, 2)
    forward(0)
    gather_for(1, 2)
    product(2, 2)
    backward(1)
    product(1, 2)
    merge(2, 2)
    complete(2, 0)
    second(1, 0)
    gather_for(0, 2)
    pass_on(0, 0)
    pass_on(2, 1)
    pass_on(1, 1)
    merge(1, 2)
    gather_for(2, 3)
    product(2, 3)
    backward(2)
    onward(1, 0)
    gather_for(1, 3)
    product(1, 3)
    merge(2, 3)
    product(0, 1)
    complete(2, 1)
    second(1, 1)
    merge(1, 3)
    pass_on(2, 2)
    pass_on(1, 2)
    merge(0, 1)
    onward(1, 1)
    complete(0, 0)
    second(0, 0)
    backward(3)
    onward(0, 0)
    complete(2, 2)
    second(1, 2)
    pass_on(2, 3)
    onward(1, 2)
    forward(1)
    pass_on(1, 3)
    product(0, 2)
    gather_for(0, 3)
    complete(2, 3)
    second(1, 3)
    pass_on(0, 1)
    product(0, 3)
    onward(1, 3)
    merge(0, 2)
    join(1, 2)
    gradient(g_up, full.at[1], acts.at[2], 0)
    merge(0, 3)
    forward(2)
    gradient(g_up, full.at[1], acts.at[2], 1)
    join(1, 3)
    for k in range(chips):
        complete(1, k)
    gradient(g_down, acts.at[1], full.at[2], 0)
    pass_on(0, 2)
    forward(3)
    complete(0, 1)
    second(0, 1)
    complete(0, 2)
    second(0, 2)
    onward(0, 1)
    pass_on(0, 3)
    onward(0, 2)
    gradient(g_down, acts.at[1], full.at[2], 1)
    collect(1)
    grad = mine[1]
    hat, inv = normal_of(xb[...].astype(F32), stats, 2, width)
    scaled = grad * gain_row[...]
    back_own[...] = lanes_of([jnp.sum(scaled, 1, keepdims=True), jnp.sum(scaled * hat, 1, keepdims=True)])
    first = [send(back_own, back_in.at[i], back_s.at[i], back_r.at[i], p) for i, p in enumerate(cols)]
    for copy in first:
        copy.start()
    lines = columns // 128
    gain_part = jnp.sum(grad * hat, 0, keepdims=True)
    for i in range(lines):
        gp_own[i : i + 1, :] = gain_part[:, i * 128 : (i + 1) * 128]
    gp_own[lines : lines + 1, :] = jnp.broadcast_to(jnp.sum(sq[...], 1, keepdims=True), (1, 128))
    gains_out = [send(gp_own, gp_in.at[row], gp_s.at[i], gp_r.at[i], p) for i, p in enumerate(rows_of)]
    for copy in gains_out:
        copy.start()
    gp_in[row] = gp_own[...]
    complete(0, 3)
    second(0, 3)
    onward(0, 3)
    join(0, 2)
    for copy in gains_out:
        copy.wait()
    gains = gp_in[0]
    for i in range(1, R):
        gains = gains + gp_in[i]
    gained[...] = gains[:lines]
    uu_own[...] = jnp.broadcast_to(gains[lines : lines + 1], (8, 128)) + jnp.sum(gains[:lines] * gains[:lines])
    fourth = [send(uu_own, uu_in.at[col], uu_s.at[i], uu_r.at[i], p) for i, p in enumerate(cols)]
    for copy in fourth:
        copy.start()
    uu_in[col] = uu_own[...]
    join(0, 3)
    for copy in first:
        copy.wait()
    sums = back_own[...]
    for i in range(C - 1):
        sums = sums + back_in[i]
    c1, c2 = sums[:, 0:1] / width, sums[:, 1:2] / width
    hat, inv = normal_of(xb[...].astype(F32), stats, 2, width)
    scaled = mine[1] * gain_row[...]
    dx[...] = (go[...].astype(F32) + inv * (scaled - c1 - hat * c2)).astype(BF16)
    for copy in fourth:
        copy.wait()
    total = uu_in[0]
    for i in range(1, C):
        total = total + uu_in[i]
    norm_value = jnp.sqrt(total)
    verdict[0] = jnp.minimum(1.0, clip_share * math.sqrt(params) / norm_value)
    verdict[1] = norm_value / math.sqrt(params)
    collect(0)
    y[...] = (xa[...].astype(F32) + mine[0]).astype(BF16)

    for j in (2, 1, 0):
        finish(mine_of[j])
        relays(j, lambda owner, sign, copies: finish(copies), range(1, chips))
        for k in range(chips):
            for i in range(6):
                passing(j, k, i).wait_send()
                for copy in hop(item(j, k), i):
                    copy.wait_send()
    for j in (0, 1):
        for i in range(chips):
            to_sib(j, i).wait_send()
            for h in range(2):
                if i == 1:
                    for copy in to_owner(j, i, h):
                        copy.wait_send()
                elif i > 1:
                    for copy in to_middle(j, i, h):
                        copy.wait_send()


def step_on_core(R, C, width, params, x_fwd, x_bwd, grad_out, gain, w_up, w_down):
    rows, columns = x_fwd.shape
    wide = w_up.shape[1]
    chips, slots = R // 2, 2 * (R // 2) - 1
    count = rows * R
    tokens, half = count // C, wide // 2
    lines = columns // 128
    VM = pltpu.VMEM
    return pl.pallas_call(
        functools.partial(step_kernel, R, C, width, params),
        out_shape=(VM((columns, wide), F32), VM((wide, columns), F32), VM((rows, columns), BF16),
                   VM((rows, columns), BF16), VM((lines, 128), F32), VM((2, 8, 128), F32)),
        in_specs=[VMEM] * 4 + [pl.BlockSpec(memory_space=pl.ANY)] * 2,
        out_specs=(VMEM,) * 6,
        scratch_shapes=[
            VM((3, count, columns), BF16), VM((3, count, wide), BF16),
            VM(w_up.shape, BF16), VM(w_down.shape, BF16), VM((1, columns), F32),
            VM((rows, 128), F32), VM((C - 1, rows, 128), F32),
            VM((6, tokens, wide), F32),
            VM((12, 6, tokens // 2, wide // C), BF16), VM((12, 6, tokens // 2, wide // C), BF16),
            VM((12, 6, 1, wide // C), F32), VM((12, 6, 1, wide // C), F32),
            VM((2, chips, 2, rows, columns), F32), VM((2, chips, rows, columns), F32),
            VM((2, chips, 2, rows, half), BF16), VM((2, 2, 2, rows, half), BF16),
            VM((2, 2, 2, rows, half), BF16), VM((2, chips, 2, 1, half), F32),
            VM((2, 2, 2, 1, half), F32), VM((2, 2, 2, 1, half), F32),
            VM((2, rows, columns), F32), VM((1, columns), F32),
            VM((rows, 128), F32), VM((C - 1, rows, 128), F32),
            VM((lines + 1, 128), F32), VM((R, lines + 1, 128), F32),
            VM((8, 128), F32), VM((C, 8, 128), F32),
        ]
        + [DMA((2,)), DMA((C - 1,)), DMA((C - 1,)),
           DMA((3, slots)), DMA((3, slots)), DMA((3, slots)), DMA((3, R))]
        + [DMA((12, 6))] * 6 + [DMA((2, chips))] * 2
        + [DMA((2, chips, 2)), DMA((2, 2, 2))] * 2 + [DMA((2, 2, 2))] * 2
        + [DMA((C - 1,))] * 2 + [DMA((R - 1,))] * 2 + [DMA((C - 1,))] * 2,
        compiler_params=pltpu.CompilerParams(
            collective_id=0, has_side_effects=True, vmem_limit_bytes=GRANT),
        cost_estimate=pl.CostEstimate(flops=2 * 10**10, bytes_accessed=10**7, transcendentals=0),
    )(x_fwd, x_bwd, grad_out, gain, w_up, w_down)


def clip_kernel(g_up, g_down, y_in, dx_in, gains, verdict, up, down, y, dx, step_gain, rms, staged, sem):
    factor = verdict[0, 0:1, 0:1]
    slots = staged.shape[1]
    size = staged.shape[2]
    for which, (grad, out) in enumerate(((g_up, up), (g_down, down))):
        for i in range(slots):
            at = pl.ds(i * size, size)
            staged[which, i] = grad[at, :] * factor
            pltpu.make_async_copy(staged.at[which, i], out.at[at, :], sem.at[which, i]).start()
    y[...] = y_in[...]
    dx[...] = dx_in[...]
    step_gain[...] = gains[...] * factor
    rms[...] = verdict[1, 0:1, 0:1]
    for which, out in enumerate((up, down)):
        for i in range(slots):
            at = pl.ds(i * size, size)
            pltpu.make_async_copy(staged.at[which, i], out.at[at, :], sem.at[which, i]).wait()


def clip(g_up, g_down, y, dx, gains, verdict):
    slots = 12
    size = g_up.shape[0] // slots
    like = jax.ShapeDtypeStruct
    return pl.pallas_call(
        clip_kernel,
        out_shape=(like(g_up.shape, F32), like(g_down.shape, F32), like(y.shape, BF16),
                   like(dx.shape, BF16), like(gains.shape, F32), like((1, 1), F32)),
        in_specs=[VMEM] * 6,
        out_specs=(pl.BlockSpec(memory_space=pl.ANY),) * 2 + (VMEM,) * 4,
        scratch_shapes=[pltpu.VMEM((2, slots, size, g_up.shape[1]), F32), DMA((2, slots))],
        compiler_params=pltpu.CompilerParams(vmem_limit_bytes=20 * 1024 * 1024),
        cost_estimate=pl.CostEstimate(flops=10**8, bytes_accessed=4 * 10**7, transcendentals=0),
    )(*(pltpu.with_memory_space_constraint(v, pltpu.VMEM) for v in (g_up, g_down, y, dx, gains, verdict)))


def with_kernels(R, C):
    def step(x_fwd, x_bwd, grad_out, gain, w_up, w_down):
        rows, columns = x_fwd.shape
        width = columns * C
        params = 2 * width * w_up.shape[1] * R + width
        parts = step_on_core(R, C, width, params, x_fwd, x_bwd, grad_out,
                             gain.reshape(columns // 128, 128), w_up, w_down)
        up, down, y, dx, step_gain, rms = clip(*parts)
        return y, dx, up, down, step_gain.reshape(columns), rms.reshape(())

    return step


def solution(mesh):
    placed = (
        P("row", "col"),
        P("row", "col"),
        P("row", "col"),
        P("col"),
        P("col", "row"),
        P("row", "col"),
    )
    R, C = mesh.shape["row"], mesh.shape["col"]
    body = with_kernels(R, C) if C == 4 and R == 8 else on_device
    return jax.shard_map(
        body,
        mesh=mesh,
        in_specs=placed,
        out_specs=(
            P("row", "col"),
            P("row", "col"),
            P("col", "row"),
            P("row", "col"),
            P("col"),
            P(),
        ),
        check_vma=False,
    )
```

```python
import functools
import math

import jax
import jax.numpy as jnp
from jax import lax
from jax.experimental import pallas as pl
from jax.experimental.pallas import tpu as pltpu
from jax.sharding import PartitionSpec as P

D = 6144
FF = 12288


eps = 1e-06
clip_share = 0.25


def erf_gelu(value):
    return 0.5 * value * (1.0 + lax.erf(value * 0.7071067811865476))


def gelu_slope(value):
    return (
        0.5 * (1.0 + lax.erf(value * 0.7071067811865476))
        + value * jnp.exp(-0.5 * value * value) * 0.3989422804014327
    )


def contract(left, right, left_dim, right_dim):
    return lax.dot_general(
        left, right, (((left_dim,), (right_dim,)), ((), ())), preferred_element_type=jnp.float32
    )


def row_sums(tokens):
    values = tokens.astype(jnp.float32)
    return (jnp.sum(values, -1), jnp.sum(values * values, -1))


def normalize(tokens, first, second):
    values = tokens.astype(jnp.float32)
    centre = first / D
    spread = second / D - centre * centre
    inv_scale = lax.rsqrt(spread + eps)
    return ((values - centre[:, None]) * inv_scale[:, None], inv_scale)


def up_both(normed_a, normed_b, w_up):
    full_a, full_b = (
        lax.all_gather(normed_a, "row", axis=0, tiled=True),
        lax.all_gather(normed_b, "row", axis=0, tiled=True),
    )
    width = w_up.shape[1]
    summed = lax.psum_scatter(
        jnp.concatenate(
            [
                jnp.dot(full_a, w_up, preferred_element_type=jnp.float32),
                jnp.dot(full_b, w_up, preferred_element_type=jnp.float32),
            ],
            1,
        ),
        "col",
        scatter_dimension=0,
        tiled=True,
    )
    return (summed[:, :width], summed[:, width:], full_b)


def on_device(x_fwd, x_bwd, grad_out, gain, w_up, w_down):
    first_a, second_a = row_sums(x_fwd)
    first_b, second_b = row_sums(x_bwd)
    first_a, second_a, first_b, second_b = lax.psum((first_a, second_a, first_b, second_b), "col")
    centred_a, _ = normalize(x_fwd, first_a, second_a)
    centred_b, inv_scale = normalize(x_bwd, first_b, second_b)
    normed_a = (centred_a * gain).astype(jnp.bfloat16)
    normed_b = (centred_b * gain).astype(jnp.bfloat16)
    pre_a, pre_b, normed_full = up_both(normed_a, normed_b, w_up)
    hidden_a = erf_gelu(pre_a).astype(jnp.bfloat16)
    output_part = jnp.dot(
        lax.all_gather(hidden_a, "col", axis=0, tiled=True),
        w_down,
        preferred_element_type=jnp.float32,
    )
    output_sum = lax.psum_scatter(output_part, "row", scatter_dimension=0, tiled=True)
    y_fwd = (x_fwd.astype(jnp.float32) + output_sum).astype(jnp.bfloat16)
    hidden_b = erf_gelu(pre_b).astype(jnp.bfloat16)
    grad_full = lax.all_gather(grad_out, "row", axis=0, tiled=True)
    grad_hidden = lax.psum_scatter(
        contract(grad_full, w_down, 1, 1), "col", scatter_dimension=0, tiled=True
    )
    grad_pre = (grad_hidden * gelu_slope(pre_b)).astype(jnp.bfloat16)
    hidden_piece = lax.all_gather(hidden_b, "col", axis=0, tiled=True)
    pre_piece = lax.all_gather(grad_pre, "col", axis=0, tiled=True)
    down_total = contract(hidden_piece, grad_full, 0, 0)
    up_total = contract(normed_full, pre_piece, 0, 0)
    input_total = contract(pre_piece, w_up, 1, 1)
    grad_normed = lax.psum_scatter(input_total, "row", scatter_dimension=0, tiled=True)
    scaled = grad_normed * gain
    first_back = jnp.sum(scaled, -1)
    second_back = jnp.sum(scaled * centred_b, -1)
    first_back, second_back = lax.psum((first_back, second_back), "col")
    dx_bwd = (
        grad_out.astype(jnp.float32)
        + inv_scale[:, None]
        * (scaled - first_back[:, None] / D - centred_b * (second_back[:, None] / D))
    ).astype(jnp.bfloat16)
    gain_part = jnp.sum(grad_normed * centred_b, 0)
    weight_squares = jnp.sum(up_total * up_total) + jnp.sum(down_total * down_total)
    g_gain = lax.psum(gain_part, "row")
    first_row = (lax.axis_index("row") == 0).astype(jnp.float32)
    total = lax.psum(weight_squares + first_row * jnp.sum(g_gain * g_gain), ("row", "col"))
    param_count = 2 * D * FF + D
    norm_value = jnp.sqrt(total)
    grad_rms = norm_value / math.sqrt(param_count)
    factor = jnp.minimum(1.0, clip_share * math.sqrt(param_count) / norm_value)
    return (y_fwd, dx_bwd, up_total * factor, down_total * factor, g_gain * factor, grad_rms)


MESH = pl.DeviceIdType.MESH
VMEM = pl.BlockSpec(memory_space=pltpu.VMEM)
F32 = jnp.float32
BF16 = jnp.bfloat16
DMA = pltpu.SemaphoreType.DMA
GRANT = 45 * 1024 * 1024


def send(src, dst, send_sem, recv_sem, peer):
    return pltpu.make_async_remote_copy(
        src_ref=src, dst_ref=dst, send_sem=send_sem, recv_sem=recv_sem,
        device_id=peer, device_id_type=MESH,
    )


def arrived(ref, sem, peer):
    pltpu.make_async_remote_copy(
        src_ref=ref, dst_ref=ref, send_sem=sem, recv_sem=sem,
        device_id=peer, device_id_type=MESH,
    ).wait_recv()


SPAN = 252.0


def encode(values):
    size = jnp.abs(values)
    peak = jnp.maximum(jnp.max(size, 0, keepdims=True), 1e-30)
    code = jnp.exp2(size * (SPAN / peak) - 0.5 * SPAN)
    return jnp.where(values < 0.0, -code, code).astype(BF16), peak


def decode(codes, peak):
    code = codes.astype(F32)
    size = jnp.log(jnp.abs(code)) * (peak * (1.4426950408889634 / SPAN)) + 0.5 * peak
    return jnp.where(code < 0.0, -size, size)


def normal_of(values, stats, at, width):
    centre = stats[:, at : at + 1] / width
    spread = stats[:, at + 1 : at + 2] / width - centre * centre
    inv = lax.rsqrt(spread + eps)
    return (values - centre) * inv, inv


def lanes_of(columns):
    rows = columns[0].shape[0]
    lane = lax.broadcasted_iota(jnp.int32, (rows, 128), 1)
    out = jnp.zeros((rows, 128), F32)
    for i, column in enumerate(columns):
        out = jnp.where(lane == i, column, out)
    return out


def step_kernel(R, C, width, params, xa, xb, go, gain, w_up_hbm, w_down_hbm,
                g_up, g_down, y, dx, gained, verdict,
                full, acts, w_up, w_down, gain_row, st_own, st_in, partial, buf, inb, buf_p, inb_p,
                part, from_sib, zbuf, zin, zmid, zbuf_p, zin_p, zmid_p, mine, sq,
                back_own, back_in, gp_own, gp_in, uu_own, uu_in,
                w_sem, st_s, st_r, s_right, s_left, s_sib, recv, hop_s, hop_r, peak_s, peak_r,
                g_s, g_r, sib_s, sib_r, z_s, z_r, zp_s, zp_r, zm_r, zmp_r,
                back_s, back_r, gp_s, gp_r, uu_s, uu_r):
    row, col = lax.axis_index("row"), lax.axis_index("col")
    chips = R // 2
    chip, core = row // 2, row % 2
    sib = {"row": row + 1 - 2 * core, "col": col}
    cols = [{"row": row, "col": (col + i) % C} for i in range(1, C)]
    rows_of = [{"row": (row + i) % R, "col": col} for i in range(1, R)]
    flip_x = col + 1 - 2 * (col % 2)
    flip_y = (col + 2) % 4
    diag = 3 - col
    peer_x, peer_y = {"row": row, "col": flip_x}, {"row": row, "col": flip_y}
    share, columns = xa.shape
    tokens = share * R // C
    wide = w_up.shape[1]
    half = wide // 2
    quarter = wide // C
    upper = tokens // 2
    tile = half // 2
    high = chip // 2

    def line(step):
        return {"row": row + 2 * step, "col": col}

    def mirror(at, on):
        return at + on * (chips - 1 - 2 * at)

    def order(k):
        low = mirror(chip, high)
        return mirror((low, 1 - low, 2, 3)[k], high)

    load_up = pltpu.make_async_copy(w_up_hbm, w_up, w_sem.at[0])
    load_down = pltpu.make_async_copy(w_down_hbm, w_down, w_sem.at[1])
    load_down.start()
    load_up.start()
    barrier = pltpu.get_barrier_semaphore()
    for peer in cols + rows_of:
        pl.semaphore_signal(barrier, inc=1, device_id=peer, device_id_type=MESH)
    moments = []
    for x in (xa, xb):
        v = x[...].astype(F32)
        moments += [jnp.sum(v, 1, keepdims=True), jnp.sum(v * v, 1, keepdims=True)]
    st_own[...] = lanes_of(moments)
    for i in range(columns // 128):
        gain_row[:, i * 128 : (i + 1) * 128] = gain[i : i + 1, :]
    sq[...] = jnp.zeros_like(sq)
    pl.semaphore_wait(barrier, len(cols) + len(rows_of))

    def block(j, owner):
        return full.at[j, pl.ds(owner * share, share), :]

    def spread(j, owner, slot, src, to_right, to_left):
        dst = block(j, owner)
        out = [(None, send(src, dst, s_sib.at[j, slot], recv.at[j, owner], sib))]
        if to_right:
            out.append((chip < chips - 1,
                        send(src, dst, s_right.at[j, slot], recv.at[j, owner], line(1))))
        if to_left:
            out.append((chip > 0,
                        send(src, dst, s_left.at[j, slot], recv.at[j, owner], line(-1))))
        return out

    def start(copies):
        for cond, copy in copies[::-1]:
            if cond is None:
                copy.start()
            else:
                pl.when(cond)(copy.start)

    def finish(copies):
        for cond, copy in copies:
            if cond is None:
                copy.wait_send()
            else:
                pl.when(cond)(copy.wait_send)

    mine_of = {2: spread(2, row, 0, go, True, True)}
    start(mine_of[2])
    st_copies = [send(st_own, st_in.at[i], st_s.at[i], st_r.at[i], p) for i, p in enumerate(cols)]
    for copy in st_copies:
        copy.start()
    block(2, row)[...] = go[...]

    def relays(j, visit, steps):
        for step in steps:
            for sign in (-1, 1):
                ok = chip >= step if sign < 0 else chip + step < chips

                @pl.when(ok)
                def _():
                    owner = row + 2 * sign * step
                    slot = step if sign < 0 else chips - 1 + step
                    visit(owner, sign, spread(j, owner, slot, block(j, owner), sign < 0, sign > 0))

    def gather(j, step):
        def visit(owner, sign, copies):
            arrived(block(j, owner), recv.at[j, owner], line(sign))
            start(copies)

        relays(j, visit, (step,))

    ends = (chip + 1) % chips < 2

    def gather_for(j, k):
        if k < 3:
            gather(j, k)
        else:
            pl.when(ends)(lambda: gather(j, 3))

    def hop(n, s):
        peer = peer_x if s in (0, 2, 3) else peer_y
        return (send(buf.at[n, s], inb.at[n, s], hop_s.at[n, s], hop_r.at[n, s], peer),
                send(buf_p.at[n, s], inb_p.at[n, s], peak_s.at[n, s], peak_r.at[n, s], peer))

    def go_hop(n, s, values):
        buf[n, s], buf_p[n, s] = encode(values)
        for copy in hop(n, s):
            copy.start()

    def got_hop(n, s):
        for copy in hop(n, s):
            copy.wait_recv()

    def over_tiles(body, size):
        @pl.loop(0, size // tile)
        def _(t):
            body(pl.ds(pl.multiple_of(t * tile, tile), tile))

    def item(j, k):
        return j * chips + k

    def place(j, k):
        return 4 + k % 2 if j == 0 else (2 * k + 2 - j) % 4

    def lanes(owner):
        return pl.ds(pl.multiple_of(owner * quarter, quarter), quarter)

    low_rows, high_rows = slice(0, upper), slice(upper, 2 * upper)

    def product(j, k):
        q = order(k)
        owner = 2 * q + 1 - core
        arrived(block(j, owner), recv.at[j, owner], sib)
        n, at_p = item(j, k), place(j, k)

        @pl.loop(0, 2)
        def _(h):
            at = pl.ds(pl.multiple_of(h * half, half), half)
            left = full[j, pl.ds(q * tokens, tokens), :]
            if j == 2:
                piece = lax.dot_general(left, w_down[at, :], (((1,), (1,)), ((), ())),
                                        preferred_element_type=F32)
            else:
                piece = jnp.dot(left, w_up[:, at], preferred_element_type=F32)
            partial[at_p, :, at] = piece

        go_hop(n, 0, partial[at_p, low_rows, lanes(diag)])
        go_hop(n, 1, partial[at_p, high_rows, lanes(diag)])
        go_hop(n, 2, partial[at_p, low_rows, lanes(flip_x)])
        go_hop(n, 5, partial[at_p, high_rows, lanes(flip_y)])

    def merge(j, k):
        n, at_p = item(j, k), place(j, k)
        got_hop(n, 0)
        go_hop(n, 4, partial[at_p, low_rows, lanes(flip_y)] + decode(inb[n, 0], inb_p[n, 0]))
        got_hop(n, 1)
        go_hop(n, 3, partial[at_p, high_rows, lanes(flip_x)] + decode(inb[n, 1], inb_p[n, 1]))

    def landed(j, k):
        for s in range(2, 6):
            got_hop(item(j, k), s)

    def summed(j, k, r, at, rows):
        n = item(j, k)
        first_s, second_s = ((2, 4), (5, 3))[r]
        return (partial[place(j, k), rows, lanes(col)]
                + decode(inb[n, first_s, at, :], inb_p[n, first_s])
                + decode(inb[n, second_s, at, :], inb_p[n, second_s]))

    chunk = 16

    def over(k, body):
        q = order(k)

        @pl.loop(0, upper // chunk)
        def _(i):
            at = pl.ds(pl.multiple_of(i * chunk, chunk), chunk)
            for r in range(2):
                rows = pl.ds(pl.multiple_of(r * upper + i * chunk, chunk), chunk)
                to = pl.ds(pl.multiple_of(q * tokens + r * upper + i * chunk, chunk), chunk)
                body(r, at, rows, to)

    def backward(k):
        landed(2, k)
        landed(1, k)

        def body(r, at, rows, to):
            v = summed(1, k, r, at, rows)
            phi = 0.5 * (1.0 + lax.erf(v * 0.7071067811865476))
            g = summed(2, k, r, at, rows)
            slope = phi + v * jnp.exp(-0.5 * v * v) * 0.3989422804014327
            acts[1, to, lanes(col)] = (v * phi).astype(BF16)
            acts[2, to, lanes(col)] = (g * slope).astype(BF16)

        over(k, body)
        publish(2, k)
        publish(1, k)

    def forward(k):
        landed(0, k)

        def body(r, at, rows, to):
            v = summed(0, k, r, at, rows)
            acts[0, to, lanes(col)] = (0.5 * v * (1.0 + lax.erf(v * 0.7071067811865476))).astype(BF16)

        over(k, body)
        publish(0, k)

    def piece_of(j, k, r, owner):
        rows = pl.ds(pl.multiple_of(order(k) * tokens + r * upper, upper), upper)
        return acts.at[j, rows, lanes(owner)]

    def passing(j, k, i):
        owner, r, peer = ((col, 0, peer_x), (col, 1, peer_y), (col, 1, peer_x), (col, 0, peer_y),
                          (flip_x, 0, peer_y), (flip_y, 1, peer_x))[i]
        ref, n = piece_of(j, k, r, owner), item(j, k)
        return send(ref, ref, g_s.at[n, i], g_r.at[n, i], peer)

    def publish(j, k):
        for i in range(4):
            passing(j, k, i).start()

    def got_piece(j, k, i):
        owner, r = ((flip_x, 0), (flip_y, 1), (flip_x, 1), (flip_y, 0), (diag, 0), (diag, 1))[i]
        arrived(piece_of(j, k, r, owner), g_r.at[item(j, k), i], peer_x)

    def pass_on(j, k):
        got_piece(j, k, 0)
        passing(j, k, 4).start()
        got_piece(j, k, 1)
        passing(j, k, 5).start()

    def complete(j, k):
        for i in range(2, 6):
            got_piece(j, k, i)

    def to_sib(j, k):
        return send(part.at[j, k, 1 - core], from_sib.at[j, k], sib_s.at[j, k], sib_r.at[j, k], sib)

    def to_owner(j, k, h):
        peer, slot = {"row": 2 * order(k) + core, "col": col}, min(k, 2) - 1
        return (send(zbuf.at[j, k, h], zin.at[j, slot, h], z_s.at[j, k, h], z_r.at[j, slot, h], peer),
                send(zbuf_p.at[j, k, h], zin_p.at[j, slot, h], zp_s.at[j, k, h], zp_r.at[j, slot, h], peer))

    def to_middle(j, k, h):
        peer = {"row": row + 2 - 4 * high, "col": col}
        return (send(zbuf.at[j, k, h], zmid.at[j, k - 2, h], z_s.at[j, k, h], zm_r.at[j, k - 2, h], peer),
                send(zbuf_p.at[j, k, h], zmid_p.at[j, k - 2, h], zp_s.at[j, k, h], zmp_r.at[j, k - 2, h], peer))

    def second(j, k):
        @pl.loop(0, 2)
        def _(h):
            at = pl.ds(pl.multiple_of(h * half, half), half)
            left = acts[2 * j, pl.ds(pl.multiple_of(order(k) * tokens, tokens), tokens), :]
            if j == 0:
                piece = jnp.dot(left, w_down[:, at], preferred_element_type=F32)
            else:
                piece = lax.dot_general(left, w_up[at, :], (((1,), (1,)), ((), ())),
                                        preferred_element_type=F32)
            part[j, k, 0, :, at] = piece[:share]
            part[j, k, 1, :, at] = piece[share:]

        to_sib(j, k).start()

    def in_half(h, at):
        return pl.ds(pl.multiple_of(h * half + at * tile, tile), tile)

    def code(j, k, h, more, copies):
        @pl.loop(0, half // tile)
        def _(t):
            at, wide_at = pl.ds(pl.multiple_of(t * tile, tile), tile), in_half(h, t)
            values = part[j, k, core, :, wide_at] + from_sib[j, k, :, wide_at]
            if more:
                values = values + decode(zmid[j, k - 2, h, :, at], zmid_p[j, k - 2, h, :, at])
            zbuf[j, k, h, :, at], zbuf_p[j, k, h, :, at] = encode(values)

        for copy in copies:
            copy.start()

    def onward(j, k):
        to_sib(j, k).wait_recv()
        if k == 0:
            mine[j] = part[j, k, core] + from_sib[j, k]
        elif k == 1:
            for h in range(2):
                code(j, k, h, False, to_owner(j, k, h))
        else:
            @pl.when(ends)
            def _():
                for h in range(2):
                    code(j, k, h, False, to_middle(j, k, h))

    def join(j, k):
        @pl.when(jnp.logical_not(ends))
        def _():
            for h in range(2):
                for copy in to_middle(j, k, h):
                    copy.wait_recv()
                code(j, k, h, True, to_owner(j, k, h))

    def collect(j):
        for slot in range(2):
            for h in range(2):
                for copy in to_owner(j, slot + 1, h):
                    copy.wait_recv()
                across = slice(h * half, (h + 1) * half)
                mine[j, :, across] = mine[j, :, across] + decode(zin[j, slot, h], zin_p[j, slot, h])

    def gradient(out, left, right, late):
        step_m, step_n = 256, half
        depth = 2 * tokens
        from_row = (high + late * (1 - 2 * high)) * depth
        rows = pl.ds(pl.multiple_of(from_row, depth), depth)

        @pl.loop(0, out.shape[0] // step_m)
        def _(m):
            at = pl.ds(pl.multiple_of(m * step_m, step_m), step_m)
            for n in range(out.shape[1] // step_n):
                across = slice(n * step_n, (n + 1) * step_n)
                piece = lax.dot_general(left[rows, at], right[rows, across], (((0,), (0,)), ((), ())),
                                        preferred_element_type=F32)
                if late:
                    piece = piece + out[at, across]
                    sq[:, across] = sq[:, across] + jnp.sum(piece * piece, 0, keepdims=True)
                out[at, across] = piece

    load_down.wait()
    product(2, 0)
    for copy in st_copies:
        copy.wait()
    stats = st_own[...]
    for i in range(C - 1):
        stats = stats + st_in[i]
    for j, x, at in ((1, xb, 2), (0, xa, 0)):
        hat, _ = normal_of(x[...].astype(F32), stats, at, width)
        block(j, row)[...] = (hat * gain_row[...]).astype(BF16)
        mine_of[j] = spread(j, row, 0, block(j, row), True, True)
        start(mine_of[j])
    load_up.wait()
    product(1, 0)
    merge(2, 0)
    product(0, 0)
    merge(1, 0)
    gather_for(2, 1)
    product(2, 1)
    backward(0)
    gather_for(1, 1)
    product(1, 1)
    merge(2, 1)
    gather_for(0, 1)
    merge(0, 0)
    pass_on(2, 0)
    pass_on(1, 0)
    merge(1, 1)
    gather_for(2, 2)
    forward(0)
    gather_for(1, 2)
    product(2, 2)
    backward(1)
    product(1, 2)
    merge(2, 2)
    complete(2, 0)
    second(1, 0)
    gather_for(0, 2)
    pass_on(0, 0)
    pass_on(2, 1)
    pass_on(1, 1)
    merge(1, 2)
    gather_for(2, 3)
    product(2, 3)
    complete(2, 1)
    gradient(g_up, full.at[1], acts.at[2], 0)
    backward(2)
    onward(1, 0)
    gather_for(1, 3)
    product(1, 3)
    merge(2, 3)
    gather_for(0, 3)
    product(0, 3)
    second(1, 1)
    merge(1, 3)
    pass_on(2, 2)
    pass_on(1, 2)
    complete(1, 0)
    complete(1, 1)
    gradient(g_down, acts.at[1], full.at[2], 0)
    merge(0, 3)
    onward(1, 1)
    complete(0, 0)
    second(0, 0)
    backward(3)
    onward(0, 0)
    complete(2, 2)
    second(1, 2)
    pass_on(2, 3)
    onward(1, 2)
    forward(3)
    pass_on(1, 3)
    product(0, 2)
    complete(2, 3)
    second(1, 3)
    pass_on(0, 3)
    product(0, 1)
    onward(1, 3)
    merge(0, 2)
    join(1, 2)
    gradient(g_up, full.at[1], acts.at[2], 1)
    complete(0, 3)
    second(0, 3)
    merge(0, 1)
    forward(2)
    onward(0, 3)
    join(1, 3)
    complete(1, 2)
    complete(1, 3)
    gradient(g_down, acts.at[1], full.at[2], 1)
    pass_on(0, 2)
    forward(1)
    join(0, 3)
    complete(0, 2)
    second(0, 2)
    pass_on(0, 1)
    onward(0, 2)
    collect(1)
    grad = mine[1]
    hat, inv = normal_of(xb[...].astype(F32), stats, 2, width)
    scaled = grad * gain_row[...]
    back_own[...] = lanes_of([jnp.sum(scaled, 1, keepdims=True), jnp.sum(scaled * hat, 1, keepdims=True)])
    first = [send(back_own, back_in.at[i], back_s.at[i], back_r.at[i], p) for i, p in enumerate(cols)]
    for copy in first:
        copy.start()
    lines = columns // 128
    gain_part = jnp.sum(grad * hat, 0, keepdims=True)
    for i in range(lines):
        gp_own[i : i + 1, :] = gain_part[:, i * 128 : (i + 1) * 128]
    gp_own[lines : lines + 1, :] = jnp.broadcast_to(jnp.sum(sq[...], 1, keepdims=True), (1, 128))
    gains_out = [send(gp_own, gp_in.at[row], gp_s.at[i], gp_r.at[i], p) for i, p in enumerate(rows_of)]
    for copy in gains_out:
        copy.start()
    gp_in[row] = gp_own[...]
    complete(0, 1)
    second(0, 1)
    onward(0, 1)
    join(0, 2)
    for copy in gains_out:
        copy.wait()
    gains = gp_in[0]
    for i in range(1, R):
        gains = gains + gp_in[i]
    gained[...] = gains[:lines]
    uu_own[...] = jnp.broadcast_to(gains[lines : lines + 1], (8, 128)) + jnp.sum(gains[:lines] * gains[:lines])
    fourth = [send(uu_own, uu_in.at[col], uu_s.at[i], uu_r.at[i], p) for i, p in enumerate(cols)]
    for copy in fourth:
        copy.start()
    uu_in[col] = uu_own[...]
    for copy in first:
        copy.wait()
    sums = back_own[...]
    for i in range(C - 1):
        sums = sums + back_in[i]
    c1, c2 = sums[:, 0:1] / width, sums[:, 1:2] / width
    hat, inv = normal_of(xb[...].astype(F32), stats, 2, width)
    scaled = mine[1] * gain_row[...]
    dx[...] = (go[...].astype(F32) + inv * (scaled - c1 - hat * c2)).astype(BF16)
    for copy in fourth:
        copy.wait()
    total = uu_in[0]
    for i in range(1, C):
        total = total + uu_in[i]
    norm_value = jnp.sqrt(total)
    verdict[0] = jnp.minimum(1.0, clip_share * math.sqrt(params) / norm_value)
    verdict[1] = norm_value / math.sqrt(params)
    collect(0)
    y[...] = (xa[...].astype(F32) + mine[0]).astype(BF16)

    for j in (2, 1, 0):
        finish(mine_of[j])
        relays(j, lambda owner, sign, copies: finish(copies), range(1, chips))
        for k in range(chips):
            for i in range(6):
                passing(j, k, i).wait_send()
                for copy in hop(item(j, k), i):
                    copy.wait_send()
    for j in (0, 1):
        for i in range(chips):
            to_sib(j, i).wait_send()
            for h in range(2):
                if i == 1:
                    for copy in to_owner(j, i, h):
                        copy.wait_send()
                elif i > 1:
                    for copy in to_middle(j, i, h):
                        copy.wait_send()


def step_on_core(R, C, width, params, x_fwd, x_bwd, grad_out, gain, w_up, w_down):
    rows, columns = x_fwd.shape
    wide = w_up.shape[1]
    chips, slots = R // 2, 2 * (R // 2) - 1
    count = rows * R
    tokens, half = count // C, wide // 2
    lines = columns // 128
    VM = pltpu.VMEM
    return pl.pallas_call(
        functools.partial(step_kernel, R, C, width, params),
        out_shape=(VM((columns, wide), F32), VM((wide, columns), F32), VM((rows, columns), BF16),
                   VM((rows, columns), BF16), VM((lines, 128), F32), VM((2, 8, 128), F32)),
        in_specs=[VMEM] * 4 + [pl.BlockSpec(memory_space=pl.ANY)] * 2,
        out_specs=(VMEM,) * 6,
        scratch_shapes=[
            VM((3, count, columns), BF16), VM((3, count, wide), BF16),
            VM(w_up.shape, BF16), VM(w_down.shape, BF16), VM((1, columns), F32),
            VM((rows, 128), F32), VM((C - 1, rows, 128), F32),
            VM((6, tokens, wide), F32),
            VM((12, 6, tokens // 2, wide // C), BF16), VM((12, 6, tokens // 2, wide // C), BF16),
            VM((12, 6, 1, wide // C), F32), VM((12, 6, 1, wide // C), F32),
            VM((2, chips, 2, rows, columns), F32), VM((2, chips, rows, columns), F32),
            VM((2, chips, 2, rows, half), BF16), VM((2, 2, 2, rows, half), BF16),
            VM((2, 2, 2, rows, half), BF16), VM((2, chips, 2, 1, half), F32),
            VM((2, 2, 2, 1, half), F32), VM((2, 2, 2, 1, half), F32),
            VM((2, rows, columns), F32), VM((1, columns), F32),
            VM((rows, 128), F32), VM((C - 1, rows, 128), F32),
            VM((lines + 1, 128), F32), VM((R, lines + 1, 128), F32),
            VM((8, 128), F32), VM((C, 8, 128), F32),
        ]
        + [DMA((2,)), DMA((C - 1,)), DMA((C - 1,)),
           DMA((3, slots)), DMA((3, slots)), DMA((3, slots)), DMA((3, R))]
        + [DMA((12, 6))] * 6 + [DMA((2, chips))] * 2
        + [DMA((2, chips, 2)), DMA((2, 2, 2))] * 2 + [DMA((2, 2, 2))] * 2
        + [DMA((C - 1,))] * 2 + [DMA((R - 1,))] * 2 + [DMA((C - 1,))] * 2,
        compiler_params=pltpu.CompilerParams(
            collective_id=0, has_side_effects=True, vmem_limit_bytes=GRANT),
        cost_estimate=pl.CostEstimate(flops=2 * 10**10, bytes_accessed=10**7, transcendentals=0),
    )(x_fwd, x_bwd, grad_out, gain, w_up, w_down)


def clip_kernel(g_up, g_down, y_in, dx_in, gains, verdict, up, down, y, dx, step_gain, rms, staged, sem):
    factor = verdict[0, 0:1, 0:1]
    slots = staged.shape[1]
    size = staged.shape[2]
    for which, (grad, out) in enumerate(((g_up, up), (g_down, down))):
        for i in range(slots):
            at = pl.ds(i * size, size)
            staged[which, i] = grad[at, :] * factor
            pltpu.make_async_copy(staged.at[which, i], out.at[at, :], sem.at[which, i]).start()
    y[...] = y_in[...]
    dx[...] = dx_in[...]
    step_gain[...] = gains[...] * factor
    rms[...] = verdict[1, 0:1, 0:1]
    for which, out in enumerate((up, down)):
        for i in range(slots):
            at = pl.ds(i * size, size)
            pltpu.make_async_copy(staged.at[which, i], out.at[at, :], sem.at[which, i]).wait()


def clip(g_up, g_down, y, dx, gains, verdict):
    slots = 12
    size = g_up.shape[0] // slots
    like = jax.ShapeDtypeStruct
    return pl.pallas_call(
        clip_kernel,
        out_shape=(like(g_up.shape, F32), like(g_down.shape, F32), like(y.shape, BF16),
                   like(dx.shape, BF16), like(gains.shape, F32), like((1, 1), F32)),
        in_specs=[VMEM] * 6,
        out_specs=(pl.BlockSpec(memory_space=pl.ANY),) * 2 + (VMEM,) * 4,
        scratch_shapes=[pltpu.VMEM((2, slots, size, g_up.shape[1]), F32), DMA((2, slots))],
        compiler_params=pltpu.CompilerParams(vmem_limit_bytes=20 * 1024 * 1024),
        cost_estimate=pl.CostEstimate(flops=10**8, bytes_accessed=4 * 10**7, transcendentals=0),
    )(*(pltpu.with_memory_space_constraint(v, pltpu.VMEM) for v in (g_up, g_down, y, dx, gains, verdict)))


def with_kernels(R, C):
    def step(x_fwd, x_bwd, grad_out, gain, w_up, w_down):
        rows, columns = x_fwd.shape
        width = columns * C
        params = 2 * width * w_up.shape[1] * R + width
        parts = step_on_core(R, C, width, params, x_fwd, x_bwd, grad_out,
                             gain.reshape(columns // 128, 128), w_up, w_down)
        up, down, y, dx, step_gain, rms = clip(*parts)
        return y, dx, up, down, step_gain.reshape(columns), rms.reshape(())

    return step


def solution(mesh):
    placed = (
        P("row", "col"),
        P("row", "col"),
        P("row", "col"),
        P("col"),
        P("col", "row"),
        P("row", "col"),
    )
    R, C = mesh.shape["row"], mesh.shape["col"]
    body = with_kernels(R, C) if C == 4 and R == 8 else on_device
    return jax.shard_map(
        body,
        mesh=mesh,
        in_specs=placed,
        out_specs=(
            P("row", "col"),
            P("row", "col"),
            P("col", "row"),
            P("row", "col"),
            P("col"),
            P(),
        ),
        check_vma=False,
    )
```

```python
import functools
import math

import jax
import jax.numpy as jnp
from jax import lax
from jax.experimental import pallas as pl
from jax.experimental.pallas import tpu as pltpu
from jax.sharding import PartitionSpec as P

D = 6144
FF = 12288


eps = 1e-06
clip_share = 0.25


def erf_gelu(value):
    return 0.5 * value * (1.0 + lax.erf(value * 0.7071067811865476))


def gelu_slope(value):
    return (
        0.5 * (1.0 + lax.erf(value * 0.7071067811865476))
        + value * jnp.exp(-0.5 * value * value) * 0.3989422804014327
    )


def contract(left, right, left_dim, right_dim):
    return lax.dot_general(
        left, right, (((left_dim,), (right_dim,)), ((), ())), preferred_element_type=jnp.float32
    )


def row_sums(tokens):
    values = tokens.astype(jnp.float32)
    return (jnp.sum(values, -1), jnp.sum(values * values, -1))


def normalize(tokens, first, second):
    values = tokens.astype(jnp.float32)
    centre = first / D
    spread = second / D - centre * centre
    inv_scale = lax.rsqrt(spread + eps)
    return ((values - centre[:, None]) * inv_scale[:, None], inv_scale)


def up_both(normed_a, normed_b, w_up):
    full_a, full_b = (
        lax.all_gather(normed_a, "row", axis=0, tiled=True),
        lax.all_gather(normed_b, "row", axis=0, tiled=True),
    )
    width = w_up.shape[1]
    summed = lax.psum_scatter(
        jnp.concatenate(
            [
                jnp.dot(full_a, w_up, preferred_element_type=jnp.float32),
                jnp.dot(full_b, w_up, preferred_element_type=jnp.float32),
            ],
            1,
        ),
        "col",
        scatter_dimension=0,
        tiled=True,
    )
    return (summed[:, :width], summed[:, width:], full_b)


def on_device(x_fwd, x_bwd, grad_out, gain, w_up, w_down):
    first_a, second_a = row_sums(x_fwd)
    first_b, second_b = row_sums(x_bwd)
    first_a, second_a, first_b, second_b = lax.psum((first_a, second_a, first_b, second_b), "col")
    centred_a, _ = normalize(x_fwd, first_a, second_a)
    centred_b, inv_scale = normalize(x_bwd, first_b, second_b)
    normed_a = (centred_a * gain).astype(jnp.bfloat16)
    normed_b = (centred_b * gain).astype(jnp.bfloat16)
    pre_a, pre_b, normed_full = up_both(normed_a, normed_b, w_up)
    hidden_a = erf_gelu(pre_a).astype(jnp.bfloat16)
    output_part = jnp.dot(
        lax.all_gather(hidden_a, "col", axis=0, tiled=True),
        w_down,
        preferred_element_type=jnp.float32,
    )
    output_sum = lax.psum_scatter(output_part, "row", scatter_dimension=0, tiled=True)
    y_fwd = (x_fwd.astype(jnp.float32) + output_sum).astype(jnp.bfloat16)
    hidden_b = erf_gelu(pre_b).astype(jnp.bfloat16)
    grad_full = lax.all_gather(grad_out, "row", axis=0, tiled=True)
    grad_hidden = lax.psum_scatter(
        contract(grad_full, w_down, 1, 1), "col", scatter_dimension=0, tiled=True
    )
    grad_pre = (grad_hidden * gelu_slope(pre_b)).astype(jnp.bfloat16)
    hidden_piece = lax.all_gather(hidden_b, "col", axis=0, tiled=True)
    pre_piece = lax.all_gather(grad_pre, "col", axis=0, tiled=True)
    down_total = contract(hidden_piece, grad_full, 0, 0)
    up_total = contract(normed_full, pre_piece, 0, 0)
    input_total = contract(pre_piece, w_up, 1, 1)
    grad_normed = lax.psum_scatter(input_total, "row", scatter_dimension=0, tiled=True)
    scaled = grad_normed * gain
    first_back = jnp.sum(scaled, -1)
    second_back = jnp.sum(scaled * centred_b, -1)
    first_back, second_back = lax.psum((first_back, second_back), "col")
    dx_bwd = (
        grad_out.astype(jnp.float32)
        + inv_scale[:, None]
        * (scaled - first_back[:, None] / D - centred_b * (second_back[:, None] / D))
    ).astype(jnp.bfloat16)
    gain_part = jnp.sum(grad_normed * centred_b, 0)
    weight_squares = jnp.sum(up_total * up_total) + jnp.sum(down_total * down_total)
    g_gain = lax.psum(gain_part, "row")
    first_row = (lax.axis_index("row") == 0).astype(jnp.float32)
    total = lax.psum(weight_squares + first_row * jnp.sum(g_gain * g_gain), ("row", "col"))
    param_count = 2 * D * FF + D
    norm_value = jnp.sqrt(total)
    grad_rms = norm_value / math.sqrt(param_count)
    factor = jnp.minimum(1.0, clip_share * math.sqrt(param_count) / norm_value)
    return (y_fwd, dx_bwd, up_total * factor, down_total * factor, g_gain * factor, grad_rms)


MESH = pl.DeviceIdType.MESH
VMEM = pl.BlockSpec(memory_space=pltpu.VMEM)
F32 = jnp.float32
BF16 = jnp.bfloat16
DMA = pltpu.SemaphoreType.DMA
GRANT = 45 * 1024 * 1024


def send(src, dst, send_sem, recv_sem, peer):
    return pltpu.make_async_remote_copy(
        src_ref=src, dst_ref=dst, send_sem=send_sem, recv_sem=recv_sem,
        device_id=peer, device_id_type=MESH,
    )


def arrived(ref, sem, peer):
    pltpu.make_async_remote_copy(
        src_ref=ref, dst_ref=ref, send_sem=sem, recv_sem=sem,
        device_id=peer, device_id_type=MESH,
    ).wait_recv()


SPAN = 252.0


def encode(values):
    size = jnp.abs(values)
    peak = jnp.maximum(jnp.max(size, 0, keepdims=True), 1e-30)
    code = jnp.exp2(size * (SPAN / peak) - 0.5 * SPAN)
    return jnp.where(values < 0.0, -code, code).astype(BF16), peak


def decode(codes, peak):
    code = codes.astype(F32)
    size = jnp.log(jnp.abs(code)) * (peak * (1.4426950408889634 / SPAN)) + 0.5 * peak
    return jnp.where(code < 0.0, -size, size)


def normal_of(values, stats, at, width):
    centre = stats[:, at : at + 1] / width
    spread = stats[:, at + 1 : at + 2] / width - centre * centre
    inv = lax.rsqrt(spread + eps)
    return (values - centre) * inv, inv


def lanes_of(columns):
    rows = columns[0].shape[0]
    lane = lax.broadcasted_iota(jnp.int32, (rows, 128), 1)
    out = jnp.zeros((rows, 128), F32)
    for i, column in enumerate(columns):
        out = jnp.where(lane == i, column, out)
    return out


def step_kernel(R, C, width, params, xa, xb, go, gain, w_up_hbm, w_down_hbm,
                g_up, g_down, y, dx, gained, verdict,
                full, acts, w_up, w_down, gain_row, st_own, st_in, partial, buf, inb, buf_p, inb_p,
                part, from_sib, zbuf, zin, zmid, zbuf_p, zin_p, zmid_p, mine, sq,
                back_own, back_in, gp_own, gp_in, uu_own, uu_in,
                w_sem, st_s, st_r, s_right, s_left, s_sib, recv, hop_s, hop_r, peak_s, peak_r,
                g_s, g_r, sib_s, sib_r, z_s, z_r, zp_s, zp_r, zm_r, zmp_r,
                back_s, back_r, gp_s, gp_r, uu_s, uu_r):
    row, col = lax.axis_index("row"), lax.axis_index("col")
    chips = R // 2
    chip, core = row // 2, row % 2
    sib = {"row": row + 1 - 2 * core, "col": col}
    cols = [{"row": row, "col": (col + i) % C} for i in range(1, C)]
    rows_of = [{"row": (row + i) % R, "col": col} for i in range(1, R)]
    flip_x = col + 1 - 2 * (col % 2)
    flip_y = (col + 2) % 4
    diag = 3 - col
    peer_x, peer_y = {"row": row, "col": flip_x}, {"row": row, "col": flip_y}
    share, columns = xa.shape
    tokens = share * R // C
    wide = w_up.shape[1]
    half = wide // 2
    quarter = wide // C
    upper = tokens // 2
    tile = half // 2
    high = chip // 2

    def line(step):
        return {"row": row + 2 * step, "col": col}

    def mirror(at, on):
        return at + on * (chips - 1 - 2 * at)

    def order(k):
        low = mirror(chip, high)
        return mirror((low, 1 - low, 2, 3)[k], high)

    load_up = pltpu.make_async_copy(w_up_hbm, w_up, w_sem.at[0])
    load_down = pltpu.make_async_copy(w_down_hbm, w_down, w_sem.at[1])
    load_down.start()
    load_up.start()
    barrier = pltpu.get_barrier_semaphore()
    for peer in cols + rows_of:
        pl.semaphore_signal(barrier, inc=1, device_id=peer, device_id_type=MESH)
    moments = []
    for x in (xa, xb):
        v = x[...].astype(F32)
        moments += [jnp.sum(v, 1, keepdims=True), jnp.sum(v * v, 1, keepdims=True)]
    st_own[...] = lanes_of(moments)
    for i in range(columns // 128):
        gain_row[:, i * 128 : (i + 1) * 128] = gain[i : i + 1, :]
    sq[...] = jnp.zeros_like(sq)
    pl.semaphore_wait(barrier, len(cols) + len(rows_of))

    def block(j, owner):
        return full.at[j, pl.ds(owner * share, share), :]

    def spread(j, owner, slot, src, to_right, to_left):
        dst = block(j, owner)
        out = [(None, send(src, dst, s_sib.at[j, slot], recv.at[j, owner], sib))]
        if to_right:
            out.append((chip < chips - 1,
                        send(src, dst, s_right.at[j, slot], recv.at[j, owner], line(1))))
        if to_left:
            out.append((chip > 0,
                        send(src, dst, s_left.at[j, slot], recv.at[j, owner], line(-1))))
        return out

    def start(copies):
        for cond, copy in copies[::-1]:
            if cond is None:
                copy.start()
            else:
                pl.when(cond)(copy.start)

    def finish(copies):
        for cond, copy in copies:
            if cond is None:
                copy.wait_send()
            else:
                pl.when(cond)(copy.wait_send)

    mine_of = {2: spread(2, row, 0, go, True, True)}
    start(mine_of[2])
    st_copies = [send(st_own, st_in.at[i], st_s.at[i], st_r.at[i], p) for i, p in enumerate(cols)]
    for copy in st_copies:
        copy.start()
    block(2, row)[...] = go[...]

    def relays(j, visit, steps):
        for step in steps:
            for sign in (-1, 1):
                ok = chip >= step if sign < 0 else chip + step < chips

                @pl.when(ok)
                def _():
                    owner = row + 2 * sign * step
                    slot = step if sign < 0 else chips - 1 + step
                    visit(owner, sign, spread(j, owner, slot, block(j, owner), sign < 0, sign > 0))

    def gather(j, step):
        def visit(owner, sign, copies):
            arrived(block(j, owner), recv.at[j, owner], line(sign))
            start(copies)

        relays(j, visit, (step,))

    ends = (chip + 1) % chips < 2

    def gather_for(j, k):
        if k < 3:
            gather(j, k)
        else:
            pl.when(ends)(lambda: gather(j, 3))

    def hop(n, s):
        peer = peer_x if s in (0, 2, 3) else peer_y
        return (send(buf.at[n, s], inb.at[n, s], hop_s.at[n, s], hop_r.at[n, s], peer),
                send(buf_p.at[n, s], inb_p.at[n, s], peak_s.at[n, s], peak_r.at[n, s], peer))

    def go_hop(n, s, values):
        buf[n, s], buf_p[n, s] = encode(values)
        for copy in hop(n, s):
            copy.start()

    def got_hop(n, s):
        for copy in hop(n, s):
            copy.wait_recv()

    def over_tiles(body, size):
        @pl.loop(0, size // tile)
        def _(t):
            body(pl.ds(pl.multiple_of(t * tile, tile), tile))

    def item(j, k):
        return j * chips + k

    def place(j, k):
        return 4 + k % 2 if j == 0 else (2 * k + 2 - j) % 4

    def lanes(owner):
        return pl.ds(pl.multiple_of(owner * quarter, quarter), quarter)

    low_rows, high_rows = slice(0, upper), slice(upper, 2 * upper)

    def product(j, k):
        q = order(k)
        owner = 2 * q + 1 - core
        arrived(block(j, owner), recv.at[j, owner], sib)
        n, at_p = item(j, k), place(j, k)

        @pl.loop(0, 2)
        def _(h):
            at = pl.ds(pl.multiple_of(h * half, half), half)
            left = full[j, pl.ds(q * tokens, tokens), :]
            if j == 2:
                piece = lax.dot_general(left, w_down[at, :], (((1,), (1,)), ((), ())),
                                        preferred_element_type=F32)
            else:
                piece = jnp.dot(left, w_up[:, at], preferred_element_type=F32)
            partial[at_p, :, at] = piece

        go_hop(n, 0, partial[at_p, low_rows, lanes(diag)])
        go_hop(n, 1, partial[at_p, high_rows, lanes(diag)])
        go_hop(n, 2, partial[at_p, low_rows, lanes(flip_x)])
        go_hop(n, 5, partial[at_p, high_rows, lanes(flip_y)])

    def merge(j, k):
        n, at_p = item(j, k), place(j, k)
        got_hop(n, 0)
        go_hop(n, 4, partial[at_p, low_rows, lanes(flip_y)] + decode(inb[n, 0], inb_p[n, 0]))
        got_hop(n, 1)
        go_hop(n, 3, partial[at_p, high_rows, lanes(flip_x)] + decode(inb[n, 1], inb_p[n, 1]))

    def landed(j, k):
        for s in range(2, 6):
            got_hop(item(j, k), s)

    def summed(j, k, r, at, rows):
        n = item(j, k)
        first_s, second_s = ((2, 4), (5, 3))[r]
        return (partial[place(j, k), rows, lanes(col)]
                + decode(inb[n, first_s, at, :], inb_p[n, first_s])
                + decode(inb[n, second_s, at, :], inb_p[n, second_s]))

    chunk = 16

    def over(k, body):
        q = order(k)

        @pl.loop(0, upper // chunk)
        def _(i):
            at = pl.ds(pl.multiple_of(i * chunk, chunk), chunk)
            for r in range(2):
                rows = pl.ds(pl.multiple_of(r * upper + i * chunk, chunk), chunk)
                to = pl.ds(pl.multiple_of(q * tokens + r * upper + i * chunk, chunk), chunk)
                body(r, at, rows, to)

    def backward(k):
        landed(2, k)
        landed(1, k)

        def body(r, at, rows, to):
            v = summed(1, k, r, at, rows)
            phi = 0.5 * (1.0 + lax.erf(v * 0.7071067811865476))
            g = summed(2, k, r, at, rows)
            slope = phi + v * jnp.exp(-0.5 * v * v) * 0.3989422804014327
            acts[1, to, lanes(col)] = (v * phi).astype(BF16)
            acts[2, to, lanes(col)] = (g * slope).astype(BF16)

        over(k, body)
        publish(2, k)
        publish(1, k)

    def forward(k):
        landed(0, k)

        def body(r, at, rows, to):
            v = summed(0, k, r, at, rows)
            acts[0, to, lanes(col)] = (0.5 * v * (1.0 + lax.erf(v * 0.7071067811865476))).astype(BF16)

        over(k, body)
        publish(0, k)

    def piece_of(j, k, r, owner):
        rows = pl.ds(pl.multiple_of(order(k) * tokens + r * upper, upper), upper)
        return acts.at[j, rows, lanes(owner)]

    def passing(j, k, i):
        owner, r, peer = ((col, 0, peer_x), (col, 1, peer_y), (col, 1, peer_x), (col, 0, peer_y),
                          (flip_x, 0, peer_y), (flip_y, 1, peer_x))[i]
        ref, n = piece_of(j, k, r, owner), item(j, k)
        return send(ref, ref, g_s.at[n, i], g_r.at[n, i], peer)

    def publish(j, k):
        for i in range(4):
            passing(j, k, i).start()

    def got_piece(j, k, i):
        owner, r = ((flip_x, 0), (flip_y, 1), (flip_x, 1), (flip_y, 0), (diag, 0), (diag, 1))[i]
        arrived(piece_of(j, k, r, owner), g_r.at[item(j, k), i], peer_x)

    def pass_on(j, k):
        got_piece(j, k, 0)
        passing(j, k, 4).start()
        got_piece(j, k, 1)
        passing(j, k, 5).start()

    def complete(j, k):
        for i in range(2, 6):
            got_piece(j, k, i)

    def to_sib(j, k):
        return send(part.at[j, k, 1 - core], from_sib.at[j, k], sib_s.at[j, k], sib_r.at[j, k], sib)

    def to_owner(j, k, h):
        peer, slot = {"row": 2 * order(k) + core, "col": col}, min(k, 2) - 1
        return (send(zbuf.at[j, k, h], zin.at[j, slot, h], z_s.at[j, k, h], z_r.at[j, slot, h], peer),
                send(zbuf_p.at[j, k, h], zin_p.at[j, slot, h], zp_s.at[j, k, h], zp_r.at[j, slot, h], peer))

    def to_middle(j, k, h):
        peer = {"row": row + 2 - 4 * high, "col": col}
        return (send(zbuf.at[j, k, h], zmid.at[j, k - 2, h], z_s.at[j, k, h], zm_r.at[j, k - 2, h], peer),
                send(zbuf_p.at[j, k, h], zmid_p.at[j, k - 2, h], zp_s.at[j, k, h], zmp_r.at[j, k - 2, h], peer))

    def second(j, k):
        @pl.loop(0, 2)
        def _(h):
            at = pl.ds(pl.multiple_of(h * half, half), half)
            left = acts[2 * j, pl.ds(pl.multiple_of(order(k) * tokens, tokens), tokens), :]
            if j == 0:
                piece = jnp.dot(left, w_down[:, at], preferred_element_type=F32)
            else:
                piece = lax.dot_general(left, w_up[at, :], (((1,), (1,)), ((), ())),
                                        preferred_element_type=F32)
            part[j, k, 0, :, at] = piece[:share]
            part[j, k, 1, :, at] = piece[share:]

        to_sib(j, k).start()

    def in_half(h, at):
        return pl.ds(pl.multiple_of(h * half + at * tile, tile), tile)

    def code(j, k, h, more, copies):
        @pl.loop(0, half // tile)
        def _(t):
            at, wide_at = pl.ds(pl.multiple_of(t * tile, tile), tile), in_half(h, t)
            values = part[j, k, core, :, wide_at] + from_sib[j, k, :, wide_at]
            if more:
                values = values + decode(zmid[j, k - 2, h, :, at], zmid_p[j, k - 2, h, :, at])
            zbuf[j, k, h, :, at], zbuf_p[j, k, h, :, at] = encode(values)

        for copy in copies:
            copy.start()

    def onward(j, k):
        to_sib(j, k).wait_recv()
        if k == 0:
            mine[j] = part[j, k, core] + from_sib[j, k]
        elif k == 1:
            for h in range(2):
                code(j, k, h, False, to_owner(j, k, h))
        else:
            @pl.when(ends)
            def _():
                for h in range(2):
                    code(j, k, h, False, to_middle(j, k, h))

    def join(j, k):
        @pl.when(jnp.logical_not(ends))
        def _():
            for h in range(2):
                for copy in to_middle(j, k, h):
                    copy.wait_recv()
                code(j, k, h, True, to_owner(j, k, h))

    def collect(j):
        for slot in range(2):
            for h in range(2):
                for copy in to_owner(j, slot + 1, h):
                    copy.wait_recv()
                across = slice(h * half, (h + 1) * half)
                mine[j, :, across] = mine[j, :, across] + decode(zin[j, slot, h], zin_p[j, slot, h])

    def gradient(out, left, right, late):
        step_m, step_n = 256, half
        depth = 2 * tokens
        from_row = (high + late * (1 - 2 * high)) * depth
        rows = pl.ds(pl.multiple_of(from_row, depth), depth)

        @pl.loop(0, out.shape[0] // step_m)
        def _(m):
            at = pl.ds(pl.multiple_of(m * step_m, step_m), step_m)
            for n in range(out.shape[1] // step_n):
                across = slice(n * step_n, (n + 1) * step_n)
                piece = lax.dot_general(left[rows, at], right[rows, across], (((0,), (0,)), ((), ())),
                                        preferred_element_type=F32)
                if late:
                    piece = piece + out[at, across]
                    sq[:, across] = sq[:, across] + jnp.sum(piece * piece, 0, keepdims=True)
                out[at, across] = piece

    load_down.wait()
    product(2, 0)
    for copy in st_copies:
        copy.wait()
    stats = st_own[...]
    for i in range(C - 1):
        stats = stats + st_in[i]
    for j, x, at in ((1, xb, 2), (0, xa, 0)):
        hat, _ = normal_of(x[...].astype(F32), stats, at, width)
        block(j, row)[...] = (hat * gain_row[...]).astype(BF16)
        mine_of[j] = spread(j, row, 0, block(j, row), True, True)
        start(mine_of[j])
    load_up.wait()
    product(1, 0)
    merge(2, 0)
    product(0, 0)
    merge(1, 0)
    gather_for(2, 1)
    product(2, 1)
    backward(0)
    gather_for(1, 1)
    product(1, 1)
    merge(2, 1)
    gather_for(0, 1)
    merge(0, 0)
    pass_on(2, 0)
    pass_on(1, 0)
    merge(1, 1)
    gather_for(2, 2)
    forward(0)
    gather_for(1, 2)
    product(2, 2)
    backward(1)
    product(1, 2)
    merge(2, 2)
    complete(2, 0)
    second(1, 0)
    gather_for(0, 2)
    pass_on(0, 0)
    pass_on(2, 1)
    pass_on(1, 1)
    merge(1, 2)
    gather_for(2, 3)
    product(2, 3)
    complete(2, 1)
    gradient(g_up, full.at[1], acts.at[2], 0)
    backward(2)
    onward(1, 0)
    gather_for(1, 3)
    product(1, 3)
    merge(2, 3)
    gather_for(0, 3)
    product(0, 3)
    second(1, 1)
    merge(1, 3)
    pass_on(2, 2)
    pass_on(1, 2)
    complete(1, 0)
    complete(1, 1)
    gradient(g_down, acts.at[1], full.at[2], 0)
    merge(0, 3)
    onward(1, 1)
    complete(0, 0)
    second(0, 0)
    backward(3)
    onward(0, 0)
    complete(2, 2)
    second(1, 2)
    pass_on(2, 3)
    onward(1, 2)
    forward(3)
    pass_on(1, 3)
    product(0, 2)
    complete(2, 3)
    second(1, 3)
    pass_on(0, 3)
    product(0, 1)
    onward(1, 3)
    merge(0, 2)
    join(1, 2)
    gradient(g_up, full.at[1], acts.at[2], 1)
    complete(0, 3)
    second(0, 3)
    merge(0, 1)
    join(1, 3)
    forward(2)
    onward(0, 3)
    complete(1, 2)
    complete(1, 3)
    gradient(g_down, acts.at[1], full.at[2], 1)
    pass_on(0, 2)
    forward(1)
    collect(1)
    grad = mine[1]
    hat, inv = normal_of(xb[...].astype(F32), stats, 2, width)
    scaled = grad * gain_row[...]
    back_own[...] = lanes_of([jnp.sum(scaled, 1, keepdims=True), jnp.sum(scaled * hat, 1, keepdims=True)])
    first = [send(back_own, back_in.at[i], back_s.at[i], back_r.at[i], p) for i, p in enumerate(cols)]
    for copy in first:
        copy.start()
    lines = columns // 128
    gain_part = jnp.sum(grad * hat, 0, keepdims=True)
    for i in range(lines):
        gp_own[i : i + 1, :] = gain_part[:, i * 128 : (i + 1) * 128]
    gp_own[lines : lines + 1, :] = jnp.broadcast_to(jnp.sum(sq[...], 1, keepdims=True), (1, 128))
    gains_out = [send(gp_own, gp_in.at[row], gp_s.at[i], gp_r.at[i], p) for i, p in enumerate(rows_of)]
    for copy in gains_out:
        copy.start()
    gp_in[row] = gp_own[...]
    join(0, 3)
    complete(0, 2)
    second(0, 2)
    pass_on(0, 1)
    onward(0, 2)
    complete(0, 1)
    second(0, 1)
    onward(0, 1)
    join(0, 2)
    for copy in gains_out:
        copy.wait()
    gains = gp_in[0]
    for i in range(1, R):
        gains = gains + gp_in[i]
    gained[...] = gains[:lines]
    uu_own[...] = jnp.broadcast_to(gains[lines : lines + 1], (8, 128)) + jnp.sum(gains[:lines] * gains[:lines])
    fourth = [send(uu_own, uu_in.at[col], uu_s.at[i], uu_r.at[i], p) for i, p in enumerate(cols)]
    for copy in fourth:
        copy.start()
    uu_in[col] = uu_own[...]
    for copy in first:
        copy.wait()
    sums = back_own[...]
    for i in range(C - 1):
        sums = sums + back_in[i]
    c1, c2 = sums[:, 0:1] / width, sums[:, 1:2] / width
    hat, inv = normal_of(xb[...].astype(F32), stats, 2, width)
    scaled = mine[1] * gain_row[...]
    dx[...] = (go[...].astype(F32) + inv * (scaled - c1 - hat * c2)).astype(BF16)
    for copy in fourth:
        copy.wait()
    total = uu_in[0]
    for i in range(1, C):
        total = total + uu_in[i]
    norm_value = jnp.sqrt(total)
    verdict[0] = jnp.minimum(1.0, clip_share * math.sqrt(params) / norm_value)
    verdict[1] = norm_value / math.sqrt(params)
    collect(0)
    y[...] = (xa[...].astype(F32) + mine[0]).astype(BF16)

    for j in (2, 1, 0):
        finish(mine_of[j])
        relays(j, lambda owner, sign, copies: finish(copies), range(1, chips))
        for k in range(chips):
            for i in range(6):
                passing(j, k, i).wait_send()
                for copy in hop(item(j, k), i):
                    copy.wait_send()
    for j in (0, 1):
        for i in range(chips):
            to_sib(j, i).wait_send()
            for h in range(2):
                if i == 1:
                    for copy in to_owner(j, i, h):
                        copy.wait_send()
                elif i > 1:
                    for copy in to_middle(j, i, h):
                        copy.wait_send()


def step_on_core(R, C, width, params, x_fwd, x_bwd, grad_out, gain, w_up, w_down):
    rows, columns = x_fwd.shape
    wide = w_up.shape[1]
    chips, slots = R // 2, 2 * (R // 2) - 1
    count = rows * R
    tokens, half = count // C, wide // 2
    lines = columns // 128
    VM = pltpu.VMEM
    return pl.pallas_call(
        functools.partial(step_kernel, R, C, width, params),
        out_shape=(VM((columns, wide), F32), VM((wide, columns), F32), VM((rows, columns), BF16),
                   VM((rows, columns), BF16), VM((lines, 128), F32), VM((2, 8, 128), F32)),
        in_specs=[VMEM] * 4 + [pl.BlockSpec(memory_space=pl.ANY)] * 2,
        out_specs=(VMEM,) * 6,
        scratch_shapes=[
            VM((3, count, columns), BF16), VM((3, count, wide), BF16),
            VM(w_up.shape, BF16), VM(w_down.shape, BF16), VM((1, columns), F32),
            VM((rows, 128), F32), VM((C - 1, rows, 128), F32),
            VM((6, tokens, wide), F32),
            VM((12, 6, tokens // 2, wide // C), BF16), VM((12, 6, tokens // 2, wide // C), BF16),
            VM((12, 6, 1, wide // C), F32), VM((12, 6, 1, wide // C), F32),
            VM((2, chips, 2, rows, columns), F32), VM((2, chips, rows, columns), F32),
            VM((2, chips, 2, rows, half), BF16), VM((2, 2, 2, rows, half), BF16),
            VM((2, 2, 2, rows, half), BF16), VM((2, chips, 2, 1, half), F32),
            VM((2, 2, 2, 1, half), F32), VM((2, 2, 2, 1, half), F32),
            VM((2, rows, columns), F32), VM((1, columns), F32),
            VM((rows, 128), F32), VM((C - 1, rows, 128), F32),
            VM((lines + 1, 128), F32), VM((R, lines + 1, 128), F32),
            VM((8, 128), F32), VM((C, 8, 128), F32),
        ]
        + [DMA((2,)), DMA((C - 1,)), DMA((C - 1,)),
           DMA((3, slots)), DMA((3, slots)), DMA((3, slots)), DMA((3, R))]
        + [DMA((12, 6))] * 6 + [DMA((2, chips))] * 2
        + [DMA((2, chips, 2)), DMA((2, 2, 2))] * 2 + [DMA((2, 2, 2))] * 2
        + [DMA((C - 1,))] * 2 + [DMA((R - 1,))] * 2 + [DMA((C - 1,))] * 2,
        compiler_params=pltpu.CompilerParams(
            collective_id=0, has_side_effects=True, vmem_limit_bytes=GRANT),
        cost_estimate=pl.CostEstimate(flops=2 * 10**10, bytes_accessed=10**7, transcendentals=0),
    )(x_fwd, x_bwd, grad_out, gain, w_up, w_down)


def clip_kernel(g_up, g_down, y_in, dx_in, gains, verdict, up, down, y, dx, step_gain, rms, staged, sem):
    factor = verdict[0, 0:1, 0:1]
    slots = staged.shape[1]
    size = staged.shape[2]
    for which, (grad, out) in enumerate(((g_up, up), (g_down, down))):
        for i in range(slots):
            at = pl.ds(i * size, size)
            staged[which, i] = grad[at, :] * factor
            pltpu.make_async_copy(staged.at[which, i], out.at[at, :], sem.at[which, i]).start()
    y[...] = y_in[...]
    dx[...] = dx_in[...]
    step_gain[...] = gains[...] * factor
    rms[...] = verdict[1, 0:1, 0:1]
    for which, out in enumerate((up, down)):
        for i in range(slots):
            at = pl.ds(i * size, size)
            pltpu.make_async_copy(staged.at[which, i], out.at[at, :], sem.at[which, i]).wait()


def clip(g_up, g_down, y, dx, gains, verdict):
    slots = 12
    size = g_up.shape[0] // slots
    like = jax.ShapeDtypeStruct
    return pl.pallas_call(
        clip_kernel,
        out_shape=(like(g_up.shape, F32), like(g_down.shape, F32), like(y.shape, BF16),
                   like(dx.shape, BF16), like(gains.shape, F32), like((1, 1), F32)),
        in_specs=[VMEM] * 6,
        out_specs=(pl.BlockSpec(memory_space=pl.ANY),) * 2 + (VMEM,) * 4,
        scratch_shapes=[pltpu.VMEM((2, slots, size, g_up.shape[1]), F32), DMA((2, slots))],
        compiler_params=pltpu.CompilerParams(vmem_limit_bytes=20 * 1024 * 1024),
        cost_estimate=pl.CostEstimate(flops=10**8, bytes_accessed=4 * 10**7, transcendentals=0),
    )(*(pltpu.with_memory_space_constraint(v, pltpu.VMEM) for v in (g_up, g_down, y, dx, gains, verdict)))


def with_kernels(R, C):
    def step(x_fwd, x_bwd, grad_out, gain, w_up, w_down):
        rows, columns = x_fwd.shape
        width = columns * C
        params = 2 * width * w_up.shape[1] * R + width
        parts = step_on_core(R, C, width, params, x_fwd, x_bwd, grad_out,
                             gain.reshape(columns // 128, 128), w_up, w_down)
        up, down, y, dx, step_gain, rms = clip(*parts)
        return y, dx, up, down, step_gain.reshape(columns), rms.reshape(())

    return step


def solution(mesh):
    placed = (
        P("row", "col"),
        P("row", "col"),
        P("row", "col"),
        P("col"),
        P("col", "row"),
        P("row", "col"),
    )
    R, C = mesh.shape["row"], mesh.shape["col"]
    body = with_kernels(R, C) if C == 4 and R == 8 else on_device
    return jax.shard_map(
        body,
        mesh=mesh,
        in_specs=placed,
        out_specs=(
            P("row", "col"),
            P("row", "col"),
            P("col", "row"),
            P("row", "col"),
            P("col"),
            P(),
        ),
        check_vma=False,
    )
```
